256 devices in a mesh: gx: 16 (over z, y_lo), gy: 4 (over x), gz: 4 (over y_hi, core).
Axes of the slice: x: 4, y: 4 (y_hi: 2, y_lo: 2; y = y_hi * 2 + y_lo), z: 8, core: 2. Of those that a mesh axis runs over, the one named last changes fastest.
Arguments:
- positions: float32 [3, 32, 8, 8, 128], P(None, 'gx', 'gy', 'gz'), may hold values from 0 to 1
- velocities: float32 [3, 32, 8, 8, 128], P(None, 'gx', 'gy', 'gz'), may hold values from -1.8 to 1.8
- pressure_prev: float32 [32, 8, 8, 128], P('gx', 'gy', 'gz'), may hold values from 0 to 0.5
- counts: int32 [32, 8, 8], P('gx', 'gy', 'gz'), may hold values from 1 to 128, as said below
- out_positions: float32 [3, 16, 4, 4, 128], P(None, 'gx', 'gy', 'gz'), may hold values from 0 to 1
- out_velocities: float32 [3, 16, 4, 4, 128], P(None, 'gx', 'gy', 'gz'), may hold values from -1.8 to 1.8
- out_dir: int32 [16, 4, 4, 128], P('gx', 'gy', 'gz'), may hold values from 0 to 5, as said below
- out_cell: int32 [16, 4, 4, 128], P('gx', 'gy', 'gz'), may hold values from 0 to 7, as said below
- out_count: int32 [16, 4, 4], P('gx', 'gy', 'gz'), may hold values from 1 to 128, as said below
Outputs:
- pressure: float32 [32, 8, 8, 128], P('gx', 'gy', 'gz')
- velocity_new: float32 [3, 32, 8, 8, 128], P(None, 'gx', 'gy', 'gz')
- density_error: float32 [2], replicated
The draws below stay inside these ranges and needn't reach their ends.
Inputs may be any that keep to these rules, and one draw needn't show every extreme that they name: `counts`: each cell's count plus the live outbox slots bound for it is at most 128. `out_dir`: 0 +x, 1 -x, 2 +y, 3 -y, 4 +z, 5 -z. `out_cell`: local index in the receiving block, of a cell on the face through which the particle enters. `out_count`: the live slots are the first ones.
All inputs are finite; a program needn't handle non-finite values.
Results may differ from the reference program's by a relative error of at most 0.0003.
Values sent between devices are 32-bit elements; how exact they have to be, the bound alone decides.
No kernel may reach another device: no remote copies, remote signals or barrier semaphores. Data moves between devices by JAX's collectives and lax.ppermute only.
A program may use at most 64 MiB of HBM per device.

```python
import jax
import jax.numpy as jnp
from jax import lax

SLOTS = 128
CX = 2
CY = 2
CZ = 2
MIGR = 128
ITERS = 2
DEVS_X = 16
DEVS_Y = 4
DEVS_Z = 4
NX = 32
NY = 8
NZ = 8


def migration_plan(key):
    root_key = jax.random.fold_in(key, 7001)
    headings = jax.random.randint(jax.random.fold_in(root_key, 1), (DEVS_X, DEVS_Y, DEVS_Z, MIGR), 0, 6)
    living = jax.random.randint(jax.random.fold_in(root_key, 2), (DEVS_X, DEVS_Y, DEVS_Z), 1, MIGR + 1)
    starts = jax.random.randint(jax.random.fold_in(root_key, 3), (DEVS_X, DEVS_Y, DEVS_Z, 6), 0, CX * CY * CZ)
    chosen = jnp.take_along_axis(starts, headings, axis=3)
    place = jnp.arange(MIGR)[None, None, None, :] + chosen
    face_x = place % (CY * CZ)
    face_y = place % (CX * CZ)
    face_z = place % (CX * CY)
    cell_x = jnp.where(headings == 0, 0, CX - 1) * CY * CZ + face_x
    cell_y = face_y // CZ * CY * CZ + jnp.where(headings == 2, 0, CY - 1) * CZ + face_y % CZ
    cell_z = face_z // CY * CY * CZ + face_z % CY * CZ + jnp.where(headings == 4, 0, CZ - 1)
    dest_cell = jnp.where(headings < 2, cell_x, jnp.where(headings < 4, cell_y, cell_z))
    return (headings, dest_cell, living)


def draw_out_dir(key, part):
    return migration_plan(key)[0].astype(jnp.int32)


def draw_out_cell(key, part):
    return migration_plan(key)[1].astype(jnp.int32)


def draw_out_count(key, part):
    return migration_plan(key)[2].astype(jnp.int32)


def draw_counts(key, part):
    headings, dest_cell, living = migration_plan(key)
    alive = jnp.arange(MIGR)[None, None, None, :] < living[..., None]
    grid_x = jnp.arange(DEVS_X)[:, None, None, None]
    grid_y = jnp.arange(DEVS_Y)[None, :, None, None]
    grid_z = jnp.arange(DEVS_Z)[None, None, :, None]
    dest_x = grid_x + jnp.where(headings == 0, 1, jnp.where(headings == 1, -1, 0))
    dest_y = grid_y + jnp.where(headings == 2, 1, jnp.where(headings == 3, -1, 0))
    dest_z = grid_z + jnp.where(headings == 4, 1, jnp.where(headings == 5, -1, 0))
    inside = (dest_x >= 0) & (dest_x < DEVS_X) & (dest_y >= 0) & (dest_y < DEVS_Y) & (dest_z >= 0) & (dest_z < DEVS_Z)
    blocks = DEVS_X * DEVS_Y * DEVS_Z
    cell_total = CX * CY * CZ
    target = ((dest_x * DEVS_Y + dest_y) * DEVS_Z + dest_z) * cell_total + dest_cell
    target = jnp.where(alive & inside, target, blocks * cell_total).reshape(-1)
    arrived = jax.ops.segment_sum(jnp.ones(target.shape, jnp.int32), target, num_segments=blocks * cell_total + 1)
    arrived = arrived[:blocks * cell_total].reshape(DEVS_X, DEVS_Y, DEVS_Z, CX, CY, CZ)
    second_key = jax.random.fold_in(key, 7002)
    extent = (DEVS_X, DEVS_Y, DEVS_Z, CX, CY, CZ)
    crowded = jax.random.randint(jax.random.fold_in(second_key, 1), extent, 1, SLOTS + 1)
    sparse = jax.random.randint(jax.random.fold_in(second_key, 2), extent, 1, SLOTS // 8 + 1)
    column = jnp.arange(DEVS_X)[:, None, None, None, None, None] * CX + jnp.arange(CX)[None, None, None, :, None, None]
    drawn = jnp.where(column * 2 < DEVS_X * CX, crowded, sparse)
    bounded = jnp.maximum(jnp.minimum(drawn, SLOTS - arrived), 1)
    return bounded.transpose(0, 3, 1, 4, 2, 5).reshape(DEVS_X * CX, DEVS_Y * CY, DEVS_Z * CZ).astype(jnp.int32)


def steps_of(stream_key, dims, cuts, least, largest):
    loudness, own = 1.0, jax.random.fold_in(stream_key, 6)
    for position, parts in cuts:
        heights = jnp.exp(jax.random.uniform(jax.random.fold_in(own, position), (parts,), jnp.float32, least / len(cuts), largest / len(cuts)))
        loudness = loudness * jnp.repeat(heights, dims[position] // parts).reshape([-1 if axis == position else 1 for axis in range(len(dims))])
    return loudness


def scatter_about(key, shape, width, reach, split=(), kind=jnp.bfloat16):
    gain = steps_of(key, shape, split, -0.22, 0.18) if split else 1.0
    values = jax.random.normal(key, shape, jnp.float32) * width * gain
    return jnp.minimum(jnp.maximum(values, -reach), reach).astype(kind)


def setup_inputs(seed: int = 0) -> dict:
    key_list = jax.random.split(jax.random.key(seed), 10)
    positions = jnp.clip(1.0 * jax.random.uniform(key_list[0], (3, NX, NY, NZ, SLOTS), jnp.float32) ** steps_of(key_list[0], (3, NX, NY, NZ, SLOTS), ((1, 16), (2, 4), (3, 4)), -0.2, 0.2), 0.0, 1.0)
    velocities = scatter_about(key_list[1], (3, NX, NY, NZ, SLOTS), 0.3, 1.8, ((1, 16), (2, 4), (3, 4)), jnp.float32)
    pressure_prev = jnp.clip(0.5 * jax.random.uniform(key_list[2], (NX, NY, NZ, SLOTS), jnp.float32) ** steps_of(key_list[2], (NX, NY, NZ, SLOTS), ((0, 16), (1, 4), (2, 4)), -0.2, 0.2), 0.0, 0.5)
    counts = draw_counts(jax.random.fold_in(key_list[9], 71), 0)
    out_positions = jnp.clip(1.0 * jax.random.uniform(key_list[4], (3, DEVS_X, DEVS_Y, DEVS_Z, MIGR), jnp.float32) ** steps_of(key_list[4], (3, DEVS_X, DEVS_Y, DEVS_Z, MIGR), ((1, 16), (2, 4), (3, 4)), -0.2, 0.2), 0.0, 1.0)
    out_velocities = scatter_about(key_list[5], (3, DEVS_X, DEVS_Y, DEVS_Z, MIGR), 0.3, 1.8, ((1, 16), (2, 4), (3, 4)), jnp.float32)
    out_dir = draw_out_dir(jax.random.fold_in(key_list[9], 71), 0)
    out_cell = draw_out_cell(jax.random.fold_in(key_list[9], 71), 0)
    out_count = draw_out_count(jax.random.fold_in(key_list[9], 71), 0)
    return dict(positions=positions, velocities=velocities, pressure_prev=pressure_prev, counts=counts, out_positions=out_positions, out_velocities=out_velocities, out_dir=out_dir, out_cell=out_cell, out_count=out_count)


kernel_var = 0.25
time_step = 2.0
particle_mass = 1.0 / 45.0
rest_density = 1.0
relaxation = 0.5
floor_value = 0.1
gravity = 0.1


def stencil_offsets():
    return [(a, b, c) for a in (-1, 0, 1) for b in (-1, 0, 1) for c in (-1, 0, 1)]


def window(padded, offset, extent):
    return padded[:, 1 + offset[0]:1 + offset[0] + extent[0], 1 + offset[1]:1 + offset[1] + extent[1], 1 + offset[2]:1 + offset[2] + extent[2], :]


def geometry(center_pos, other_pos, offset):
    deltas = [center_pos[k][..., :, None] - other_pos[k][..., None, :] - float(offset[k]) for k in range(3)]
    distance = deltas[0] * deltas[0] + deltas[1] * deltas[1] + deltas[2] * deltas[2]
    kernel = jnp.exp(-distance / kernel_var)
    factor = (-2.0 / kernel_var) * kernel
    return kernel, [factor * d for d in deltas]


def setup_pass(center_pos, center_vel, near_pos, near_vel, near_mass):
    extent = center_pos.shape[1:4]
    zeros = jnp.zeros(center_pos.shape[1:], jnp.float32)
    density, divergence, grad_square = zeros, zeros, zeros
    grad_sum = [zeros, zeros, zeros]
    for offset in stencil_offsets():
        other_pos = window(near_pos, offset, extent)
        other_vel = window(near_vel, offset, extent)
        masses = window(near_mass, offset, extent)[0][..., None, :]
        kernel, grads = geometry(center_pos, other_pos, offset)
        density = density + jnp.sum(masses * kernel, -1)
        closing = sum((center_vel[k][..., :, None] - other_vel[k][..., None, :]) * grads[k] for k in range(3))
        divergence = divergence + jnp.sum(masses * closing, -1)
        grad_sum = [grad_sum[k] + jnp.sum(masses * grads[k], -1) for k in range(3)]
        grad_square = grad_square + jnp.sum(masses * (grads[0] * grads[0] + grads[1] * grads[1] + grads[2] * grads[2]), -1)
    return jnp.stack([density, divergence, grad_sum[0], grad_sum[1], grad_sum[2], grad_square])


def accel_pass(center_pos, center_scaled, near_pos, near_mass, near_scaled):
    extent = center_pos.shape[1:4]
    zeros = jnp.zeros(center_pos.shape[1:], jnp.float32)
    totals = [zeros, zeros, zeros]
    for offset in stencil_offsets():
        other_pos = window(near_pos, offset, extent)
        masses = window(near_mass, offset, extent)[0][..., None, :]
        others = window(near_scaled, offset, extent)[0][..., None, :]
        kernel, grads = geometry(center_pos, other_pos, offset)
        factor = masses * (center_scaled[0][..., :, None] + others)
        totals = [totals[k] + jnp.sum(factor * grads[k], -1) for k in range(3)]
    return -jnp.stack(totals)


def apply_pass(center_pos, center_acc, near_pos, near_mass, near_acc):
    extent = center_pos.shape[1:4]
    total = jnp.zeros(center_pos.shape[1:], jnp.float32)
    for offset in stencil_offsets():
        other_pos = window(near_pos, offset, extent)
        masses = window(near_mass, offset, extent)[0][..., None, :]
        other_acc = window(near_acc, offset, extent)
        kernel, grads = geometry(center_pos, other_pos, offset)
        closing = sum((center_acc[k][..., :, None] - other_acc[k][..., None, :]) * grads[k] for k in range(3))
        total = total + jnp.sum(masses * closing, -1)
    return (time_step * time_step * total)[None]


def payloads(out_positions, out_velocities, out_dir, out_cell, out_count):
    migrants = out_dir.shape[-1]
    living = jnp.arange(migrants, dtype=jnp.int32) < out_count[..., None]
    cargo = jnp.concatenate([out_positions, out_velocities], 0)
    result = []
    for d in range(6):
        tagged = jnp.where(living & (out_dir == d), out_cell + 1, 0).astype(jnp.float32)
        result.append(jnp.concatenate([cargo, tagged[None]], 0))
    return result


def insert(particle_state, counts, arrivals):
    cell_total = counts.size
    slots = particle_state.shape[-1]
    flat_state = particle_state.reshape(6, cell_total * slots)
    filled = counts.reshape(cell_total)
    tagged = arrivals[6].astype(jnp.int32) - 1
    onehot = (tagged[:, None] == jnp.arange(cell_total, dtype=jnp.int32)[None, :]).astype(jnp.int32)
    ranked = jnp.cumsum(onehot, 0, dtype=jnp.int32) - onehot
    start = jnp.sum(onehot * filled[None, :], 1, dtype=jnp.int32)
    within = jnp.sum(onehot * ranked, 1, dtype=jnp.int32)
    target = jnp.where(tagged >= 0, tagged * slots + start + within, cell_total * slots).astype(jnp.int32)
    placed = jax.ops.segment_sum(arrivals[:6].T, target, num_segments=cell_total * slots + 1)[:cell_total * slots].T
    slot_index = jnp.arange(slots, dtype=jnp.int32)
    kept = (slot_index[None, :] < filled[:, None]).reshape(cell_total * slots)
    merged = jnp.where(kept[None, :], flat_state, placed)
    grown = filled + jnp.sum(onehot, 0, dtype=jnp.int32)
    return merged.reshape(particle_state.shape), grown.reshape(counts.shape)


def displaced(array, axis, direction):
    length = array.shape[axis]
    widths = [(0, 0)] * array.ndim
    widths[axis] = (1, 0) if direction > 0 else (0, 1)
    padded = jnp.pad(array, widths)
    if direction > 0:
        return lax.slice_in_dim(padded, 0, length, axis=axis)
    return lax.slice_in_dim(padded, 1, length + 1, axis=axis)


def global_pass(passing, centers, paddeds):
    def single(index):
        center_parts = [lax.dynamic_slice_in_dim(c, index, 1, 1) for c in centers]
        padded_parts = [lax.dynamic_slice_in_dim(p, index, 3, 1) for p in paddeds]
        return passing(*center_parts, *padded_parts)

    stacked = lax.map(single, jnp.arange(centers[0].shape[1], dtype=jnp.int32))
    return jnp.moveaxis(stacked[:, :, 0], 0, 1)


def padding(array):
    return jnp.pad(array, ((0, 0), (1, 1), (1, 1), (1, 1), (0, 0)))


def reference(positions, velocities, pressure_prev, counts, out_positions, out_velocities, out_dir, out_cell, out_count):
    devices = DEVS_X * DEVS_Y * DEVS_Z
    cargo = payloads(out_positions, out_velocities, out_dir, out_cell, out_count)
    received = [displaced(cargo[d], 1 + d // 2, 1 if d % 2 == 0 else -1) for d in range(6)]
    arrivals = jnp.concatenate(received, -1).transpose(1, 2, 3, 0, 4).reshape(devices, 7, -1)
    joined = jnp.concatenate([positions, velocities], 0)
    blocks = joined.reshape(6, DEVS_X, CX, DEVS_Y, CY, DEVS_Z, CZ, SLOTS).transpose(1, 3, 5, 0, 2, 4, 6, 7).reshape(devices, 6, CX, CY, CZ, SLOTS)
    block_counts = counts.reshape(DEVS_X, CX, DEVS_Y, CY, DEVS_Z, CZ).transpose(0, 2, 4, 1, 3, 5).reshape(devices, CX, CY, CZ)
    state_blocks, count_blocks = lax.map(lambda t: insert(t[0], t[1], t[2]), (blocks, block_counts, arrivals))
    particle_state = state_blocks.reshape(DEVS_X, DEVS_Y, DEVS_Z, 6, CX, CY, CZ, SLOTS).transpose(3, 0, 4, 1, 5, 2, 6, 7).reshape(6, NX, NY, NZ, SLOTS)
    new_counts = count_blocks.reshape(DEVS_X, DEVS_Y, DEVS_Z, CX, CY, CZ).transpose(0, 3, 1, 4, 2, 5).reshape(NX, NY, NZ)
    slot_index = jnp.arange(SLOTS, dtype=jnp.int32)
    occupied = slot_index < new_counts[..., None]
    was_there = slot_index < counts[..., None]
    masses = jnp.where(occupied, particle_mass, 0.0).astype(jnp.float32)[None]
    local_pos = particle_state[0:3]
    local_vel = particle_state[3:6]
    pos_padded = padding(local_pos)
    mass_padded = padding(masses)
    summary = global_pass(setup_pass, [local_pos, local_vel], [pos_padded, padding(local_vel), mass_padded])
    density, divergence, grad_square = summary[0], summary[1], summary[5]
    safe = jnp.where(occupied, density, 1.0)
    source = jnp.where(occupied, rest_density - (density + time_step * divergence), 0.0)
    grad_norm = summary[2] * summary[2] + summary[3] * summary[3] + summary[4] * summary[4]
    diagonal = jnp.maximum(time_step * time_step * (grad_norm + masses[0] * grad_square) / (safe * safe), floor_value)
    pressure = jnp.where(was_there, pressure_prev, 0.0)
    errors = []
    for _ in range(ITERS):
        scaled = jnp.where(occupied, pressure / (safe * safe), 0.0)[None]
        accel = global_pass(accel_pass, [local_pos, scaled], [pos_padded, mass_padded, padding(scaled)])
        applied = global_pass(apply_pass, [local_pos, accel], [pos_padded, mass_padded, padding(accel)])[0]
        residual = jnp.where(occupied, source - applied, 0.0)
        errors.append(jnp.sum(jnp.abs(residual)) / (NX * NY * NZ * SLOTS))
        pressure = jnp.where(occupied, jnp.maximum(pressure + relaxation * (applied - source) / diagonal, 0.0), 0.0)
    scaled = jnp.where(occupied, pressure / (safe * safe), 0.0)[None]
    accel = global_pass(accel_pass, [local_pos, scaled], [pos_padded, mass_padded, padding(scaled)])
    pulled = accel + jnp.array([0.0, 0.0, -gravity], jnp.float32)[:, None, None, None, None]
    velocity_new = jnp.where(occupied[None], local_vel + time_step * pulled, 0.0)
    return pressure, velocity_new, jnp.stack(errors)
```

```python
import math

import jax
import jax.numpy as jnp
from jax import lax
from jax.experimental import pallas as pl
from jax.experimental.pallas import tpu as pltpu
from jax.sharding import PartitionSpec as P

ITERS = 2
PLANE = ("gy", "gz")
F32 = jnp.float32
BF16 = jnp.bfloat16

kernel_var = 0.25
time_step = 2.0
particle_mass = 1.0 / 45.0
rest_density = 1.0
relaxation = 0.5
floor_value = 0.1
gravity = 0.1

KAPPA = math.log2(math.e) / kernel_var
YSCALE = math.sqrt(2.0 * KAPPA)
GRAD = 2.0 / kernel_var
ABSENT = 30000.0
PADDED = ((-1, 1), (0, 0), (0, 1), (1, 0))
VMEM = pl.BlockSpec(memory_space=pltpu.VMEM)
SMEM = pl.BlockSpec(memory_space=pltpu.SMEM)


def rows_iota(shape):
    return lax.broadcasted_iota(jnp.int32, shape, 0)


def split3(x):
    h = x.astype(BF16).astype(F32)
    m = (x - h).astype(BF16).astype(F32)
    return h, m, x - h - m


def stacked(x):
    h, m, l = split3(x)
    return jnp.concatenate([h, m, l, jnp.zeros_like(x)], 0).astype(BF16)


def unstacked(acc):
    return acc[0:8] + acc[8:16] + acc[16:24]


def dot(a, b):
    return jnp.dot(a, b, preferred_element_type=F32)


def plane_source(idx, dy, dz):
    gy = idx[1] + dy
    gz = idx[2] + dz
    ok = (gy >= 0) & (gy < idx[3]) & (gz >= 0) & (gz < idx[4])
    return jnp.where(ok, gy * idx[4] + gz, 0), ok


def pack_kernel(cnt, pos, vel, heading, cell, send, one):
    lane = lax.broadcasted_iota(jnp.int32, (1, 128), 1)
    code = jnp.where(lane < cnt[0, 0, 0], heading[0, 0] * 8 + cell[0, 0] + 1, 0).astype(F32)
    one[0:1, :] = code
    for f in range(3):
        one[1 + f : 2 + f, :] = pos[f, 0, 0]
        one[4 + f : 5 + f, :] = vel[f, 0, 0]
    one[7:8, :] = jnp.zeros((1, 128), F32)
    tile = one[...]
    for p in range(send.shape[0]):
        send[p] = tile


def insert_kernel(idx, cnt, recv, xlo, xhi, pos, vel, send, base):
    row = rows_iota((8, 128))
    lane = lax.broadcasted_iota(jnp.int32, (8, 128), 1)
    cargos, marks = [], []
    for d in range(6):
        if d < 2:
            tile, ok = (xlo, xhi)[d][...], True
        else:
            step = -1 if d % 2 == 0 else 1
            src, ok = plane_source(idx, step if d < 4 else 0, step if d >= 4 else 0)
            tile = recv[src]
        mark = tile[0:1] == (row + (d * 8 + 1)).astype(F32)
        if ok is not True:
            mark = mark & ok
        cargos.append(stacked(tile))
        marks.append(jnp.where(mark, 1.0, 0.0))
    marked = jnp.concatenate(marks, 0).astype(BF16)
    r128 = rows_iota((128, 128))
    c128 = lax.broadcasted_iota(jnp.int32, (128, 128), 1)
    before = dot(marked, jnp.where(r128 < c128, 1.0, 0.0).astype(BF16))
    total = dot(marked, jnp.ones((128, 128), BF16))
    filled = jnp.zeros((8, 128), jnp.int32)
    for c in range(8):
        filled = jnp.where(row == c, cnt[c // 4, c // 2 % 2, c % 2], filled)
    grown = filled.astype(F32)
    targets = []
    for d in range(6):
        targets.append(jnp.where(marks[d] > 0, before[d * 8 : d * 8 + 8] + grown, -1.0))
        grown = grown + total[d * 8 : d * 8 + 8]
    slot = r128.astype(F32)
    lanef = lane.astype(F32)
    for c in range(8):
        acc = jnp.zeros((32, 128), F32)
        for d in range(6):
            hot = jnp.where(slot == targets[d][c : c + 1], 1.0, 0.0).astype(BF16)
            acc = acc + lax.dot_general(
                cargos[d], hot, (((1,), (1,)), ((), ())), preferred_element_type=F32
            )
        for f in range(3):
            base[c, 1 + f : 2 + f, :] = pos[f, c // 4, c // 2 % 2, c % 2 : c % 2 + 1, :]
            base[c, 4 + f : 5 + f, :] = vel[f, c // 4, c // 2 % 2, c % 2 : c % 2 + 1, :]
        base[c, 0:1, :] = jnp.zeros((1, 128), F32)
        base[c, 7:8, :] = jnp.zeros((1, 128), F32)
        tile = jnp.where(lane < cnt[c // 4, c // 2 % 2, c % 2], base[c], unstacked(acc))
        occ = lanef < grown[c : c + 1]
        tile = jnp.where(row == 0, 1.0, jnp.where(row == 7, 0.0, tile))
        tile = jnp.where(occ, tile, 0.0)
        for p in range(send.shape[0]):
            send[p, c] = tile


def gather_kernel(idx, recv, low, high):
    for yp, (dy, y) in enumerate(PADDED):
        for zp, (dz, z) in enumerate(PADDED):
            src, ok = plane_source(idx, dy, dz)
            q = yp * 4 + zp
            for x, out in enumerate((low, high)):
                c = x * 4 + y * 2 + z
                if len(recv.shape) == 3:
                    out[q : q + 1, :] = jnp.where(ok, recv[src, c : c + 1, :], 0.0)
                else:
                    out[q] = jnp.where(ok, recv[src, c], 0.0)


def gather_last_kernel(idx, recv, send, low, high):
    gather_kernel(idx, recv, low, high)
    totals = recv[0, 8:16, :]
    for p in range(1, recv.shape[0]):
        totals = totals + recv[p, 8:16, :]
    a0, a1 = low[...], high[...]
    for p in range(send.shape[0]):
        send[p, 0:16, :] = jnp.where(p > idx[0], a1, a0)
        send[p, 16:24, :] = totals


def setup_kernel(idx, cnt, p0, p1, p2, p3, pprev, whi, wlo, xr, own, aux, press, send, tiles, at, bi, ft, srow):
    row = rows_iota((8, 128))
    axis_row = (row >= 1) & (row <= 3)
    for x, ref in enumerate((p0, p1, p2, p3)):
        tiles[x * 16 : x * 16 + 16] = ref[...]
    ones_rows = jnp.where((row >= 3) & (row < 6), 1.0, 0.0)
    minus_rows = jnp.where(row < 3, -1.0, 0.0)
    zeros8 = jnp.zeros((8, 128), F32)

    def column(xy, carry):
        xs = (xy // 4 - 2).astype(F32)
        ys = (xy % 4 - 2).astype(F32)
        for z in range(4):
            tile = tiles[xy * 4 + z]
            occ = tile[0:1]
            shift = jnp.where(row == 1, xs, jnp.where(row == 2, ys, jnp.where(row == 3, z - 2.0, 0.0)))
            st = (tile + shift) * occ
            tiles[xy * 4 + z] = st
            xr[xy * 4 + z] = jnp.where(row < 4, st, 0.0)
            vel = pltpu.roll(st, 5, 0)
            vx = jnp.sum(jnp.where(axis_row, st * vel, 0.0), 0, keepdims=True)
            ft[xy, :, z * 128 : z * 128 + 128] = stacked(jnp.where(row == 7, vx, st))
            y = jnp.where(axis_row, st * YSCALE, 0.0)
            q = 0.5 * jnp.sum(y * y, 0, keepdims=True)
            h, m, l = split3(y)
            qj = jnp.where(occ > 0, q, ABSENT)
            jh, jm, jl = split3(qj)
            qcol = jnp.where(row == 0, jh, jnp.where(row == 1, jm, jnp.where(row == 2, jl, ones_rows)))
            side = jnp.concatenate([h, h, m, m, h, l, qcol, zeros8], 0)
            at[xy, z * 128 : z * 128 + 128, :] = side.T.astype(BF16)
            ih, im, il = split3(q)
            qrow = jnp.where(row == 3, -ih, jnp.where(row == 4, -im, jnp.where(row == 5, -il, minus_rows)))
            bi[xy * 4 + z] = jnp.concatenate([h, m, h, m, l, h, qrow, zeros8], 0).astype(BF16)
        return carry

    lax.fori_loop(0, 16, column, 0)

    def centre(cxy, carry):
        cx, cy = cxy // 2, cxy % 2
        for cz in range(2):
            c = cxy * 2 + cz
            q = ((cx + 1) * 4 + cy + 1) * 4 + cz + 1
            b = bi[q]
            acc = jnp.zeros((32, 128), F32)
            gs = jnp.zeros((8, 128), F32)
            for ab in range(9):
                xy = (cx + ab // 3) * 4 + cy + ab % 3
                e = dot(at[xy, cz * 128 : cz * 128 + 384, :], b)
                w = jnp.exp2(e)
                hi = w.astype(BF16)
                lo = (w - hi.astype(F32)).astype(BF16)
                whi[cxy, cz, ab] = hi
                wlo[cxy, cz, ab] = lo
                f = ft[xy, :, cz * 128 : cz * 128 + 384]
                acc = acc + dot(f, hi) + dot(f, lo)
                gs = gs + jnp.sum((w * w * e).reshape(48, 8, 128), 0)
            r = unstacked(acc)
            st = tiles[q]
            occ = st[0:1] > 0
            s0 = r[0:1]
            g = jnp.where(axis_row, st * s0 - r, 0.0)
            own[c] = g
            density = particle_mass * s0
            pair = pltpu.roll(st, 5, 0) * g - st * pltpu.roll(r, 5, 0)
            divergence = (-GRAD * particle_mass) * (
                jnp.sum(jnp.where(axis_row, pair, 0.0), 0, keepdims=True) + r[7:8]
            )
            grad_norm = (GRAD * particle_mass) ** 2 * jnp.sum(g * g, 0, keepdims=True)
            grad_square = (-GRAD * GRAD * particle_mass / KAPPA) * jnp.sum(gs, 0, keepdims=True)
            safe = jnp.where(occ, density, 1.0)
            safe2 = safe * safe
            source = jnp.where(occ, rest_density - (density + time_step * divergence), 0.0)
            weight = jnp.where(occ, particle_mass, 0.0)
            diagonal = jnp.maximum(
                time_step * time_step * (grad_norm + weight * grad_square) / safe2, floor_value
            )
            lane = lax.broadcasted_iota(jnp.int32, (1, 128), 1)
            pressure = jnp.where(lane < cnt[cx, cy, cz], pprev[cx, cy, cz : cz + 1, :], 0.0)
            aux[c, 0:1, :] = safe2
            aux[c, 1:2, :] = source
            aux[c, 2:3, :] = diagonal
            press[pl.ds(c, 1), :] = pressure
            srow[pl.ds(c, 1), :] = jnp.where(occ, pressure / safe2, 0.0)
        return carry

    lax.fori_loop(0, 4, centre, 0)
    tile = srow[...]
    for p in range(send.shape[0]):
        send[p] = tile


def pass_over(whi, wlo, ft, finish):
    def centre(cxy, carry):
        cx, cy = cxy // 2, cxy % 2
        for cz in range(2):
            acc = jnp.zeros((32, 128), F32)
            for ab in range(9):
                f = ft[(cx + ab // 3) * 4 + cy + ab % 3, :, cz * 128 : cz * 128 + 384]
                acc = acc + dot(f, whi[cxy, cz, ab]) + dot(f, wlo[cxy, cz, ab])
            finish(cx, cy, cz, ((cx + 1) * 4 + cy + 1) * 4 + cz + 1, unstacked(acc))
        return carry

    lax.fori_loop(0, 4, centre, 0)


def scaled_features(planes, xr, ft, srows):
    for x, ref in enumerate(planes):
        srows[x * 16 : x * 16 + 16, :] = ref[...]

    def column(xy, carry):
        for z in range(4):
            q = xy * 4 + z
            ft[xy, :, z * 128 : z * 128 + 128] = stacked(srows[pl.ds(q, 1), :] * xr[q])
        return carry

    lax.fori_loop(0, 16, column, 0)


def accel_of(q, c, r, srows, xr, own):
    return (GRAD * particle_mass) * (srows[pl.ds(q, 1), :] * own[c] + xr[q] * r[0:1] - r)


def accel_kernel(p0, p1, p2, p3, xr, own, whi, wlo, send, ft, srows):
    scaled_features((p0, p1, p2, p3), xr, ft, srows)

    def finish(cx, cy, cz, q, r):
        c = (cx * 2 + cy) * 2 + cz
        a = accel_of(q, c, r, srows, xr, own)[0:4]
        for p in range(send.shape[0]):
            send[p, c] = a

    pass_over(whi, wlo, ft, finish)


def apply_kernel(p0, p1, p2, p3, xr, own, whi, wlo, aux, press, errs, pnew, enew, send, ft, tiles, *, at_iter, last):
    row = rows_iota((8, 128))
    axis_row = (row >= 1) & (row <= 3)
    zeros4 = jnp.zeros((4, 128), F32)

    for x, ref in enumerate((p0, p1, p2, p3)):
        tiles[x * 16 : x * 16 + 16] = ref[...]

    def column(xy, carry):
        for z in range(4):
            q = xy * 4 + z
            a = jnp.concatenate([tiles[q], zeros4], 0)
            ax = jnp.sum(jnp.where(axis_row, a * xr[q], 0.0), 0, keepdims=True)
            ft[xy, :, z * 128 : z * 128 + 128] = stacked(jnp.where(row == 0, ax, a))
        return carry

    lax.fori_loop(0, 16, column, 0)
    enew[...] = errs[...]

    def finish(cx, cy, cz, q, r):
        c = (cx * 2 + cy) * 2 + cz
        a = jnp.concatenate([tiles[q], zeros4], 0)
        x = xr[q]
        inner = jnp.sum(jnp.where(axis_row, a * own[c] - x * r, 0.0), 0, keepdims=True) + r[0:1]
        applied = (-time_step * time_step * GRAD * particle_mass) * inner
        occ = x[0:1] > 0
        safe2, source, diagonal = (aux[c, k : k + 1, :] for k in range(3))
        residual = jnp.where(occ, source - applied, 0.0)
        enew[at_iter : at_iter + 1, :] = enew[at_iter : at_iter + 1, :] + jnp.abs(residual)
        p = press[pl.ds(c, 1), :]
        p = jnp.where(occ, jnp.maximum(p + relaxation * (applied - source) / diagonal, 0.0), 0.0)
        scaled = jnp.where(occ, p / safe2, 0.0)
        if last:
            pnew[cx, cy, cz : cz + 1, :] = p
        else:
            pnew[pl.ds(c, 1), :] = p
        send[0, pl.ds(c, 1), :] = scaled

    pass_over(whi, wlo, ft, finish)
    if last:
        send[0, 8:16, :] = enew[...]
    tile = send[0]
    for p in range(1, send.shape[0]):
        send[p] = tile


def final_kernel(idx, recv, p1, p2, state, xr, own, whi, wlo, vout, eout, ft, srows, *, slots):
    gx, nx = idx[0], recv.shape[0]
    totals = recv[0, 16:24, :]
    for p in range(1, nx):
        totals = totals + recv[p, 16:24, :]
    for it in range(ITERS):
        eout[it] = jnp.sum(totals[it : it + 1, :]) / slots
    low = jnp.where(gx > 0, recv[jnp.maximum(gx - 1, 0), 0:16, :], 0.0)
    high = jnp.where(gx < nx - 1, recv[jnp.minimum(gx + 1, nx - 1), 0:16, :], 0.0)
    scaled_features((low, p1, p2, high), xr, ft, srows)
    row = rows_iota((8, 128))

    def finish(cx, cy, cz, q, r):
        c = (cx * 2 + cy) * 2 + cz
        a = accel_of(q, c, r, srows, xr, own)
        st = state[0, c]
        pulled = a - jnp.where(row == 3, gravity, 0.0)
        v = pltpu.roll(st, 5, 0) + time_step * pulled
        v = jnp.where(st[0:1] > 0, v, 0.0)
        for f in range(3):
            vout[f, cx, cy, cz : cz + 1, :] = v[1 + f : 2 + f]

    pass_over(whi, wlo, ft, finish)


def call(body, outs, specs, scratch=(), limit=24 << 20):
    params = pltpu.CompilerParams(vmem_limit_bytes=limit)
    return pl.pallas_call(
        body,
        out_shape=outs,
        in_specs=specs,
        out_specs=jax.tree.map(lambda o: SMEM if o.shape == (ITERS,) else VMEM, outs),
        scratch_shapes=list(scratch),
        compiler_params=params,
    )


def sds(*shape, dtype=F32):
    return jax.ShapeDtypeStruct(shape, dtype)


def on_device(positions, velocities, pressure_prev, counts, out_positions, out_velocities, out_dir, out_cell, out_count):
    nx, ny, nz = lax.axis_size("gx"), lax.axis_size("gy"), lax.axis_size("gz")
    plane = ny * nz
    idx = jnp.stack([lax.axis_index("gx"), lax.axis_index("gy"), lax.axis_index("gz"), ny, nz]).astype(jnp.int32)
    forward = [(i, i + 1) for i in range(nx - 1)]
    backward = [(b, a) for a, b in forward]

    def spread(send):
        return lax.all_to_all(send, PLANE, 0, 0)

    def beside(a0, a1):
        return lax.ppermute(a1, "gx", forward), lax.ppermute(a0, "gx", backward)

    def planes(send, shape):
        a0, a1 = call(gather_kernel, (sds(16, *shape), sds(16, *shape)), [SMEM, VMEM])(idx, spread(send))
        low, high = beside(a0, a1)
        return low, a0, a1, high

    send, one = call(pack_kernel, (sds(plane, 8, 128), sds(8, 128)), [SMEM] + [VMEM] * 4)(
        out_count, out_positions, out_velocities, out_dir, out_cell
    )
    xlo, xhi = beside(one, one)
    send = call(
        insert_kernel, sds(plane, 8, 8, 128), [SMEM, SMEM] + [VMEM] * 5, [pltpu.VMEM((8, 8, 128), F32)]
    )(idx, counts, spread(send), xlo, xhi, positions, velocities)
    state = send
    near = planes(send, (8, 128))
    wshape = sds(4, 2, 9, 384, 128, dtype=BF16)
    ft = pltpu.VMEM((16, 32, 512), BF16)
    whi, wlo, xr, own, aux, press, send = call(
        setup_kernel,
        (wshape, wshape, sds(64, 8, 128), sds(8, 8, 128), sds(8, 8, 128), sds(8, 128), sds(plane, 8, 128)),
        [SMEM, SMEM] + [VMEM] * 5,
        [pltpu.VMEM((64, 8, 128), F32), pltpu.VMEM((16, 512, 64), BF16), pltpu.VMEM((64, 64, 128), BF16), ft, pltpu.VMEM((8, 128), F32)],
    )(idx, counts, *near, pressure_prev)
    errs = jnp.zeros((8, 128), F32)
    for it in range(ITERS):
        last = it == ITERS - 1
        near = planes(send, (128,))
        send = call(accel_kernel, sds(plane, 8, 4, 128), [VMEM] * 8, [ft, pltpu.VMEM((64, 128), F32)])(
            *near, xr, own, whi, wlo
        )
        near = planes(send, (4, 128))

        def body(*refs, it=it, last=last):
            apply_kernel(*refs, at_iter=it, last=last)

        press, errs, send = call(
            body,
            (sds(2, 2, 2, 128) if last else sds(8, 128), sds(8, 128), sds(plane, 16 if last else 8, 128)),
            [VMEM] * 11,
            [ft, pltpu.VMEM((64, 4, 128), F32)],
        )(*near, xr, own, whi, wlo, aux, press, errs)
    send, a0, a1 = call(gather_last_kernel, (sds(nx, 24, 128), sds(16, 128), sds(16, 128)), [SMEM, VMEM])(
        idx, spread(send)
    )
    recv = lax.all_to_all(send, "gx", 0, 0)
    slots = nx * plane * 8 * 128

    def body(*refs):
        final_kernel(*refs, slots=slots)

    velocity_new, density_error = call(
        body, (sds(3, 2, 2, 2, 128), sds(ITERS)), [SMEM] + [VMEM] * 8, [ft, pltpu.VMEM((64, 128), F32)]
    )(idx, recv, a0, a1, state, xr, own, whi, wlo)
    return press, velocity_new, density_error


def solution(mesh):
    cells = P("gx", "gy", "gz", None)
    vectors = P(None, "gx", "gy", "gz", None)
    ints = P("gx", "gy", "gz")
    return jax.shard_map(
        on_device,
        mesh=mesh,
        in_specs=(vectors, vectors, cells, ints, vectors, vectors, cells, cells, ints),
        out_specs=(cells, vectors, P()),
        check_vma=False,
    )
```

```python
import math

import jax
import jax.numpy as jnp
from jax import lax
from jax.experimental import pallas as pl
from jax.experimental.pallas import tpu as pltpu
from jax.sharding import Mesh
from jax.sharding import PartitionSpec as P

ITERS = 2
GROUP = ("gx1", "gy", "gz")
F32 = jnp.float32
BF16 = jnp.bfloat16

kernel_var = 0.25
time_step = 2.0
particle_mass = 1.0 / 45.0
rest_density = 1.0
relaxation = 0.5
floor_value = 0.1
gravity = 0.1

KAPPA = math.log2(math.e) / kernel_var
YSCALE = math.sqrt(2.0 * KAPPA)
GRAD = 2.0 / kernel_var
ABSENT = 30000.0
PADDED = ((-1, 1), (0, 0), (0, 1), (1, 0))
VMEM = pl.BlockSpec(memory_space=pltpu.VMEM)
SMEM = pl.BlockSpec(memory_space=pltpu.SMEM)


def rows_iota(shape):
    return lax.broadcasted_iota(jnp.int32, shape, 0)


def split3(x):
    h = x.astype(BF16).astype(F32)
    m = (x - h).astype(BF16).astype(F32)
    return h, m, x - h - m


def stacked(x):
    h, m, l = split3(x)
    return jnp.concatenate([h, m, l, jnp.zeros_like(x)], 0).astype(BF16)


def unstacked(acc):
    return acc[0:8] + acc[8:16] + acc[16:24]


def dot(a, b):
    return jnp.dot(a, b, preferred_element_type=F32)


def plane_source(dy, dz):
    ny, nz = lax.axis_size("gy"), lax.axis_size("gz")
    y, z = lax.axis_index("gy"), lax.axis_index("gz")
    ok = (y + dy >= 0) & (y + dy < ny) & (z + dz >= 0) & (z + dz < nz)
    return jnp.where(ok, (y + dy) * nz + z + dz, y * nz + z), ok


def plane_start(other):
    g = lax.axis_index("gx1")
    return (1 - g if other else g) * (lax.axis_size("gy") * lax.axis_size("gz"))


def outer_x(x):
    g = lax.axis_index("gx1")
    return g if x == 0 else 1 - g


def pack_kernel(count, pos, vel, heading, cell, send, one):
    lane = lax.broadcasted_iota(jnp.int32, (1, 128), 1)
    code = jnp.where(lane < count[0, 0, 0], heading[0, 0] * 8 + cell[0, 0] + 1, 0).astype(F32)
    one[0:1, :] = code
    for f in range(3):
        one[1 + f : 2 + f, :] = pos[f, 0, 0]
        one[4 + f : 5 + f, :] = vel[f, 0, 0]
    one[7:8, :] = jnp.zeros((1, 128), F32)
    tile = one[...]
    for p in range(send.shape[0]):
        send[p] = tile


def prepare_kernel(pos, vel, pprev, counts, base, before, filled):
    lane2 = lax.broadcasted_iota(jnp.int32, (1, 2), 1)
    for c in range(8):
        x, y, z = outer_x(c // 4), c // 2 % 2, c % 2
        base[c, 0:1, :] = jnp.zeros((1, 128), F32)
        base[c, 7:8, :] = jnp.zeros((1, 128), F32)
        for f in range(3):
            base[c, 1 + f : 2 + f, :] = pos[f, x, y, z : z + 1, :]
            base[c, 4 + f : 5 + f, :] = vel[f, x, y, z : z + 1, :]
        before[c : c + 1, :] = pprev[x, y, z : z + 1, :]
        pair = counts[x, y : y + 1, :].astype(F32)
        count = jnp.sum(jnp.where(lane2 == z, pair, 0.0), 1, keepdims=True)
        filled[c : c + 1, :] = jnp.broadcast_to(count, (1, 128))


def fill_chunks(send, cell_of, rows):
    def put(p, cells):
        for k, c in enumerate(cells):
            if rows:
                send[p, k] = cell_of(c)
            else:
                send[p, k : k + 1, :] = cell_of(c)

    for p in range(send.shape[0]):
        put(p, range(4, 8))
    here = plane_start(False)
    for dy in (-1, 0, 1):
        for dz in (-1, 0, 1):
            if dy or dz:
                src, _ = plane_source(dy, dz)
                face = max(dz if dz else dy, 0)
                cells = [x * 4 + (k * 2 + face if dz else face * 2 + k) for x in range(2) for k in range(2)]
                put(here + src, cells)


def gather_kernel(recv, mine, l1, l2, near, far=None):
    here, there = plane_start(False), plane_start(True)
    whole = len(mine.shape) == 3

    def read(ref, p, k):
        return ref[p, k] if whole else ref[p, k : k + 1, :]

    for yp, (dy, y) in enumerate(PADDED):
        for zp, (dz, z) in enumerate(PADDED):
            src, ok = plane_source(dy, dz)
            q = yp * 4 + zp
            outs = [(near, jnp.where(ok, read(recv, there + src, y * 2 + z), 0.0))]
            if far is not None:
                outs.append((far, jnp.where(ok, read(recv, there + src, 4 + y * 2 + z), 0.0)))
            for x, out in enumerate((l1, l2)):
                if dy == 0 and dz == 0:
                    c = x * 4 + y * 2 + z
                    value = mine[c] if whole else mine[c : c + 1, :]
                else:
                    value = jnp.where(ok, read(recv, here + src, x * 2 + (y if dz else z)), 0.0)
                outs.append((out, value))
            for out, value in outs:
                if whole:
                    out[q] = value
                else:
                    out[q : q + 1, :] = value


def gather_last_kernel(recv, mine, send, l1, l2, near, far):
    gather_kernel(recv, mine, l1, l2, near, far)
    totals = recv[0, 8:16, :]
    for p in range(1, recv.shape[0]):
        totals = totals + recv[p, 8:16, :]
    layer = far[...]
    for p in range(send.shape[0]):
        send[p, 0:16, :] = layer
        send[p, 16:24, :] = totals


def insert_kernel(recv, beyond, base, counts, send, state):
    row = rows_iota((8, 128))
    lanef = lax.broadcasted_iota(jnp.int32, (8, 128), 1).astype(F32)
    here, there = plane_start(False), plane_start(True)
    g = lax.axis_index("gx1")
    cell = row + 4 * g - jnp.where(row >= 4, 8 * g, 0)
    cargos, marks = [], []
    for d in range(6):
        step = -1 if d % 2 == 0 else 1
        if d < 2:
            src, ok = plane_source(0, 0)
            tile = jnp.where(g == d, beyond[...], recv[there + src])
        else:
            src, ok = plane_source(step if d < 4 else 0, step if d >= 4 else 0)
            tile = recv[here + src]
        mark = (tile[0:1] == (cell + (d * 8 + 1)).astype(F32)) & ok
        cargos.append(stacked(tile))
        marks.append(jnp.where(mark, 1.0, 0.0))
    marked = jnp.concatenate(marks, 0).astype(BF16)
    r128 = rows_iota((128, 128))
    c128 = lax.broadcasted_iota(jnp.int32, (128, 128), 1)
    earlier = dot(marked, jnp.where(r128 < c128, 1.0, 0.0).astype(BF16))
    total = dot(marked, jnp.ones((128, 128), BF16))
    filled = counts[...]
    grown = filled
    targets = []
    for d in range(6):
        targets.append(jnp.where(marks[d] > 0, earlier[d * 8 : d * 8 + 8] + grown, -1.0))
        grown = grown + total[d * 8 : d * 8 + 8]
    slot = r128.astype(F32)
    for c in range(8):
        acc = jnp.zeros((32, 128), F32)
        for d in range(6):
            hot = jnp.where(slot == targets[d][c : c + 1], 1.0, 0.0).astype(BF16)
            acc = acc + lax.dot_general(
                cargos[d], hot, (((1,), (1,)), ((), ())), preferred_element_type=F32
            )
        tile = jnp.where(lanef < filled[c : c + 1], base[c], unstacked(acc))
        occ = lanef < grown[c : c + 1]
        tile = jnp.where(row == 0, 1.0, jnp.where(row == 7, 0.0, tile))
        state[c] = jnp.where(occ, tile, 0.0)
    fill_chunks(send, lambda c: state[c], True)


def column_features(xy, z, tile, xs, ys, xr, at, ft):
    row = rows_iota((8, 128))
    axis_row = (row >= 1) & (row <= 3)
    occ = tile[0:1]
    shift = jnp.where(row == 1, xs, jnp.where(row == 2, ys, jnp.where(row == 3, z - 2.0, 0.0)))
    st = (tile + shift) * occ
    xr[xy * 4 + z] = jnp.where(row < 4, st, 0.0)
    vx = jnp.sum(jnp.where(axis_row, st * pltpu.roll(st, 5, 0), 0.0), 0, keepdims=True)
    ft[xy, :, z * 128 : z * 128 + 128] = stacked(jnp.where(row == 7, vx, st))
    y = jnp.where(axis_row, st * YSCALE, 0.0)
    h, m, l = split3(y)
    qh, qm, ql = split3(jnp.where(occ > 0, 0.5 * jnp.sum(y * y, 0, keepdims=True), ABSENT))
    ones_rows = jnp.where((row >= 3) & (row < 6), 1.0, 0.0)
    qcol = jnp.where(row == 0, qh, jnp.where(row == 1, qm, jnp.where(row == 2, ql, ones_rows)))
    side = jnp.concatenate([h, h, m, m, h, l, qcol, jnp.zeros((8, 128), F32)], 0)
    at[xy, z * 128 : z * 128 + 128, :] = side.T.astype(BF16)
    return st


def centre_side(st):
    row = rows_iota((8, 128))
    y = jnp.where((row >= 1) & (row <= 3), st * YSCALE, 0.0)
    h, m, l = split3(y)
    qh, qm, ql = split3(0.5 * jnp.sum(y * y, 0, keepdims=True))
    minus_rows = jnp.where(row < 3, -1.0, 0.0)
    qrow = jnp.where(row == 3, -qh, jnp.where(row == 4, -qm, jnp.where(row == 5, -ql, minus_rows)))
    return jnp.concatenate([h, m, h, m, l, h, qrow, jnp.zeros((8, 128), F32)], 0).astype(BF16)


def weigh(side, b, put):
    inner = dot(side(128, 384), b)
    pieces = (
        (0, 0, dot(side(0, 128), b[:, 0:128])),
        (0, 128, inner[:, 0:128]),
        (1, 0, inner[:, 128:256]),
        (1, 256, dot(side(384, 512), b[:, 128:256])),
    )
    sums = [jnp.zeros((8, 128), F32), jnp.zeros((8, 128), F32)]
    for cz, k, e in pieces:
        w = jnp.exp2(e)
        hi = w.astype(BF16)
        put(cz, k, k + e.shape[0], hi, (w - hi.astype(F32)).astype(BF16))
        sums[cz] = sums[cz] + jnp.sum((w * w * e).reshape(e.shape[0] // 8, 8, 128), 0)
    return sums


def main_columns(cx):
    if cx == 0:
        return [(k, k // 3, k % 3) for k in range(6)]
    return [(6 + k, k // 3, k % 3) for k in range(9)]


def setup_main_kernel(l1, l2, near, whi, wlo, xr, own, bside, part, gpart, at, bi, ft):
    g = lax.axis_index("gx1")
    for x, ref in enumerate((l1, l2, near)):
        xs = jnp.where(g == 0, x - 1.0, -1.0 * x)

        def column(y, carry, x=x, ref=ref, xs=xs):
            for z in range(4):
                column_features(x * 4 + y, z, ref[y * 4 + z], xs, (y - 2).astype(F32), xr, at, ft)
            return carry

        lax.fori_loop(0, 4, column, 0)
    row = rows_iota((8, 128))
    for c in range(8):
        cx, cy, cz = c // 4, c // 2 % 2, c % 2
        tile = (l1, l2)[cx][(cy + 1) * 4 + cz + 1]
        xs = jnp.where(g == 0, cx - 1.0, -1.0 * cx)
        shift = jnp.where(row == 1, xs, jnp.where(row == 2, cy - 1.0, jnp.where(row == 3, cz - 1.0, 0.0)))
        st = (tile + shift) * tile[0:1]
        own[c] = st
        bi[c // 2, :, cz * 128 : cz * 128 + 128] = centre_side(st)
    bside[...] = bi[0:2]

    def weights(cy, carry):
        for cx in range(2):
            b = bi[cx * 2 + cy]
            sums = [jnp.zeros((8, 128), F32), jnp.zeros((8, 128), F32)]
            for k, x, y in main_columns(cx):
                xy = x * 4 + cy + y

                def put(cz, lo, hi, a, b, k=k):
                    whi[cy, cz, k, lo:hi, :] = a
                    wlo[cy, cz, k, lo:hi, :] = b

                more = weigh(lambda lo, hi, xy=xy: at[xy, lo:hi, :], b, put)
                sums = [p + q for p, q in zip(sums, more)]
            for cz in range(2):
                gpart[(cx * 2 + cy) * 2 + cz] = sums[cz]
        return carry

    lax.fori_loop(0, 2, weights, 0)
    main_pass(whi, wlo, ft, part)


def main_pass(whi, wlo, ft, part):
    def centre(cy, carry):
        for cx in range(2):
            for cz in range(2):
                acc = jnp.zeros((32, 128), F32)
                for k, x, y in main_columns(cx):
                    f = ft[x * 4 + cy + y, :, cz * 128 : cz * 128 + 384]
                    acc = acc + dot(f, whi[cy, cz, k]) + dot(f, wlo[cy, cz, k])
                part[(cx * 2 + cy) * 2 + cz] = unstacked(acc)
        return carry

    lax.fori_loop(0, 2, centre, 0)


def beyond_pass(whi, wlo, ft, part, finish):
    for c in range(8):
        cx, cy, cz = c // 4, c // 2 % 2, c % 2
        r = part[c]
        if cx == 0:
            acc = jnp.zeros((32, 128), F32)
            for y in range(3):
                f = ft[cy + y, :, cz * 128 : cz * 128 + 384]
                acc = acc + dot(f, whi[cy, cz, y]) + dot(f, wlo[cy, cz, y])
            r = r + unstacked(acc)
        finish(c, r)


def setup_beyond_kernel(beyond, own, bside, part, gpart, counts, pprev, whi, wlo, xr, grad, aux, press, send, srow, at, ft, gsq):
    g = lax.axis_index("gx1")
    row = rows_iota((8, 128))
    axis_row = (row >= 1) & (row <= 3)
    xs = jnp.where(g == 0, -2.0, 1.0)
    for y in range(4):
        for z in range(4):
            column_features(y, z, beyond[y * 4 + z], xs, y - 2.0, xr, at, ft)
    gsq[...] = gpart[...]
    for cy in range(2):
        for y in range(3):

            def put(cz, lo, hi, a, b, cy=cy, y=y):
                whi[cy, cz, y, lo:hi, :] = a
                wlo[cy, cz, y, lo:hi, :] = b

            more = weigh(lambda lo, hi, xy=cy + y: at[xy, lo:hi, :], bside[cy], put)
            for cz in range(2):
                gsq[cy * 2 + cz] = gsq[cy * 2 + cz] + more[cz]

    def finish(c, r):
        st = own[c]
        occ = st[0:1] > 0
        s0 = r[0:1]
        gr = jnp.where(axis_row, st * s0 - r, 0.0)
        grad[c] = gr
        density = particle_mass * s0
        pair = pltpu.roll(st, 5, 0) * gr - st * pltpu.roll(r, 5, 0)
        divergence = (-GRAD * particle_mass) * (
            jnp.sum(jnp.where(axis_row, pair, 0.0), 0, keepdims=True) + r[7:8]
        )
        grad_norm = (GRAD * particle_mass) ** 2 * jnp.sum(gr * gr, 0, keepdims=True)
        grad_square = (-GRAD * GRAD * particle_mass / KAPPA) * jnp.sum(gsq[c], 0, keepdims=True)
        safe = jnp.where(occ, density, 1.0)
        safe2 = safe * safe
        source = jnp.where(occ, rest_density - (density + time_step * divergence), 0.0)
        weight = jnp.where(occ, particle_mass, 0.0)
        diagonal = jnp.maximum(
            time_step * time_step * (grad_norm + weight * grad_square) / safe2, floor_value
        )
        lane = lax.broadcasted_iota(jnp.int32, (1, 128), 1).astype(F32)
        pressure = jnp.where(lane < counts[c : c + 1, :], pprev[c : c + 1, :], 0.0)
        aux[c, 0:1, :] = safe2
        aux[c, 1:2, :] = source
        aux[c, 2:3, :] = diagonal
        press[c : c + 1, :] = pressure
        srow[c : c + 1, :] = jnp.where(occ, pressure / safe2, 0.0)

    beyond_pass(whi, wlo, ft, part, finish)
    fill_chunks(send, lambda c: srow[c : c + 1, :], False)


def scaled_features(layer, base, xr, ft):
    for y in range(4):
        for z in range(4):
            q = y * 4 + z
            ft[base // 4 + y, :, z * 128 : z * 128 + 128] = stacked(layer[q : q + 1, :] * xr[base + q])


def accel_features(layer, base, xr, ft):
    row = rows_iota((8, 128))
    axis_row = (row >= 1) & (row <= 3)
    zeros4 = jnp.zeros((4, 128), F32)
    for y in range(4):
        for z in range(4):
            q = y * 4 + z
            a = jnp.concatenate([layer[q], zeros4], 0)
            ax = jnp.sum(jnp.where(axis_row, a * xr[base + q], 0.0), 0, keepdims=True)
            ft[base // 4 + y, :, z * 128 : z * 128 + 128] = stacked(jnp.where(row == 0, ax, a))


def main_kernel(l1, l2, near, xr, whi, wlo, part, ft, *, features):
    for x, layer in enumerate((l1, l2, near)):
        features(layer, x * 16, xr, ft)
    main_pass(whi, wlo, ft, part)


def own_row(c):
    return (c // 2 % 2 + 1) * 4 + c % 2 + 1


def accel_of(c, r, l1, l2, xr, grad):
    q = own_row(c)
    s = (l1, l2)[c // 4][q : q + 1, :]
    return (GRAD * particle_mass) * (s * grad[c] + xr[c // 4 * 16 + q] * r[0:1] - r)


def accel_kernel(beyond, xrb, whi, wlo, part, l1, l2, xr, grad, send, mine, ft):
    scaled_features(beyond, 0, xrb, ft)

    def finish(c, r):
        mine[c] = accel_of(c, r, l1, l2, xr, grad)[0:4]

    beyond_pass(whi, wlo, ft, part, finish)
    fill_chunks(send, lambda c: mine[c], True)


def apply_kernel(beyond, xrb, whi, wlo, part, l1, l2, xr, grad, aux, press, errs, pnew, enew, send, mine, ft, *, at_iter, last):
    row = rows_iota((8, 128))
    axis_row = (row >= 1) & (row <= 3)
    zeros4 = jnp.zeros((4, 128), F32)
    accel_features(beyond, 0, xrb, ft)
    enew[...] = jnp.zeros((8, 128), F32) if errs is None else errs[...]

    def finish(c, r):
        q = own_row(c)
        a = jnp.concatenate([(l1, l2)[c // 4][q], zeros4], 0)
        x = xr[c // 4 * 16 + q]
        inner = jnp.sum(jnp.where(axis_row, a * grad[c] - x * r, 0.0), 0, keepdims=True) + r[0:1]
        applied = (-time_step * time_step * GRAD * particle_mass) * inner
        occ = x[0:1] > 0
        safe2, source, diagonal = (aux[c, k : k + 1, :] for k in range(3))
        residual = jnp.where(occ, source - applied, 0.0)
        enew[at_iter : at_iter + 1, :] = enew[at_iter : at_iter + 1, :] + jnp.abs(residual)
        p = press[c : c + 1, :]
        p = jnp.where(occ, jnp.maximum(p + relaxation * (applied - source) / diagonal, 0.0), 0.0)
        if last:
            pnew[outer_x(c // 4), c // 2 % 2, c % 2 : c % 2 + 1, :] = p
        else:
            pnew[c : c + 1, :] = p
        mine[c : c + 1, :] = jnp.where(occ, p / safe2, 0.0)

    beyond_pass(whi, wlo, ft, part, finish)
    fill_chunks(send, lambda c: mine[c : c + 1, :], False)
    if last:
        first, totals = mine[0:4, :], enew[...]
        for p in range(send.shape[0]):
            send[p, 4:8, :] = first
            send[p, 8:16, :] = totals


def final_kernel(recv, xrb, whi, wlo, part, l1, l2, xr, grad, state, vout, eout, beyond, ft, *, slots):
    n = recv.shape[0]
    totals = recv[0, 16:24, :]
    for p in range(1, n):
        totals = totals + recv[p, 16:24, :]
    for it in range(ITERS):
        eout[it] = jnp.sum(totals[it : it + 1, :]) / slots
    src = lax.axis_index("gx0") + 2 * lax.axis_index("gx1") - 1
    ok = (src >= 0) & (src < n)
    beyond[...] = jnp.where(ok, recv[jnp.where(ok, src, 0), 0:16, :], 0.0)
    scaled_features(beyond, 0, xrb, ft)
    row = rows_iota((8, 128))

    def finish(c, r):
        a = accel_of(c, r, l1, l2, xr, grad)
        st = state[c]
        pulled = a - jnp.where(row == 3, gravity, 0.0)
        v = pltpu.roll(st, 5, 0) + time_step * pulled
        v = jnp.where(st[0:1] > 0, v, 0.0)
        for f in range(3):
            vout[f, outer_x(c // 4), c // 2 % 2, c % 2 : c % 2 + 1, :] = v[1 + f : 2 + f]

    beyond_pass(whi, wlo, ft, part, finish)


def call(body, outs, operands, scratch=(), limit=12 << 20, flops=0, first=None, **static):
    def named(*refs):
        body(*refs, **static)

    specs = [VMEM] * len(operands)
    if first is not None:
        specs[0] = first
    return pl.pallas_call(
        named,
        out_shape=outs,
        in_specs=specs,
        out_specs=jax.tree.map(lambda o: SMEM if o.shape == (ITERS,) else VMEM, outs),
        scratch_shapes=list(scratch),
        compiler_params=pltpu.CompilerParams(vmem_limit_bytes=limit),
        cost_estimate=pl.CostEstimate(flops=flops, transcendentals=0, bytes_accessed=0) if flops else None,
    )(*operands)


def sds(*shape, dtype=F32):
    return jax.ShapeDtypeStruct(shape, dtype)


def on_device(positions, velocities, pressure_prev, counts, out_positions, out_velocities, out_dir, out_cell, out_count):
    pairs, plane = lax.axis_size("gx0"), lax.axis_size("gy") * lax.axis_size("gz")
    group = 2 * plane
    across = [(2 * j + 1, 2 * j + 2) for j in range(pairs - 1)]
    across = across + [(b, a) for a, b in across]
    busy = 4 * 10**9

    def spread(send):
        return lax.all_to_all(send, GROUP, 0, 0)

    def from_beyond(layer):
        return lax.ppermute(layer, ("gx0", "gx1"), across)

    def layers(send, mine, shape):
        return call(gather_kernel, (sds(16, *shape),) * 3, (spread(send), mine))

    def features(columns):
        return pltpu.VMEM((columns, 32, 512), BF16)

    tiles, rows = sds(8, 8, 128), sds(8, 128)
    send, one = call(
        pack_kernel,
        (sds(group, 8, 128), rows),
        (out_count, out_positions, out_velocities, out_dir, out_cell),
        limit=60 * 1024 * 1024,
        first=SMEM,
    )
    base, before, filled = call(
        prepare_kernel, (tiles, rows, rows), (positions, velocities, pressure_prev, counts), flops=busy // 4
    )
    send, state = call(insert_kernel, (sds(group, 4, 8, 128), tiles), (spread(send), from_beyond(one), base, filled))
    l1, l2, near = layers(send, state, (8, 128))
    beyond = from_beyond(l1)
    wmain, wside = sds(2, 2, 15, 384, 128, dtype=BF16), sds(2, 2, 3, 384, 128, dtype=BF16)
    whi, wlo, xr, own, bside, part, gpart = call(
        setup_main_kernel,
        (wmain, wmain, sds(48, 8, 128), tiles, sds(2, 64, 256, dtype=BF16), tiles, tiles),
        (l1, l2, near),
        [pltpu.VMEM((12, 512, 64), BF16), pltpu.VMEM((4, 64, 256), BF16), features(12)],
        flops=3 * busy,
    )
    bhi, blo, xrb, grad, aux, press, send, mine = call(
        setup_beyond_kernel,
        (wside, wside, sds(16, 8, 128), tiles, tiles, rows, sds(group, 4, 128), rows),
        (beyond, own, bside, part, gpart, filled, before),
        [pltpu.VMEM((4, 512, 64), BF16), features(4), pltpu.VMEM((8, 8, 128), F32)],
    )
    errs = None
    for it in range(ITERS):
        last = it == ITERS - 1
        l1, l2, near = layers(send, mine, (128,))
        beyond = from_beyond(l1)
        (part,) = call(
            main_kernel, (tiles,), (l1, l2, near, xr, whi, wlo), [features(12)], flops=busy, features=scaled_features
        )
        send, mine = call(
            accel_kernel,
            (sds(group, 4, 4, 128), sds(8, 4, 128)),
            (beyond, xrb, bhi, blo, part, l1, l2, xr, grad),
            [features(4)],
        )
        l1, l2, near = layers(send, mine, (4, 128))
        beyond = from_beyond(l1)
        (part,) = call(
            main_kernel, (tiles,), (l1, l2, near, xr, whi, wlo), [features(12)], flops=busy, features=accel_features
        )

        def body(*refs, it=it, last=last):
            refs = refs if it else (*refs[:11], None, *refs[11:])
            apply_kernel(*refs, at_iter=it, last=last)

        operands = (beyond, xrb, bhi, blo, part, l1, l2, xr, grad, aux, press) + (() if it == 0 else (errs,))
        press, errs, send, mine = call(
            body,
            (sds(2, 2, 2, 128) if last else rows, rows, sds(group, 16 if last else 4, 128), rows),
            operands,
            [features(4)],
        )
    send, l1, l2, near, _ = call(
        gather_last_kernel, (sds(pairs, 24, 128),) + (sds(16, 128),) * 4, (spread(send), mine)
    )
    recv = lax.all_to_all(send, "gx0", 0, 0)
    (part,) = call(
        main_kernel, (tiles,), (l1, l2, near, xr, whi, wlo), [features(12)], flops=busy, features=scaled_features
    )
    velocity_new, density_error = call(
        final_kernel,
        (sds(3, 2, 2, 2, 128), sds(ITERS)),
        (recv, xrb, bhi, blo, part, l1, l2, xr, grad, state),
        [pltpu.VMEM((16, 128), F32), features(4)],
        slots=pairs * group * 8 * 128,
    )
    return press, velocity_new, density_error


def solution(mesh):
    nx, ny, nz = (mesh.shape[a] for a in ("gx", "gy", "gz"))
    paired = Mesh(mesh.devices.reshape(nx // 2, 2, ny, nz), ("gx0", "gx1", "gy", "gz"))
    gx = ("gx0", "gx1")
    cells = P(gx, "gy", "gz", None)
    vectors = P(None, gx, "gy", "gz", None)
    ints = P(gx, "gy", "gz")
    return jax.shard_map(
        on_device,
        mesh=paired,
        in_specs=(vectors, vectors, cells, ints, vectors, vectors, cells, cells, ints),
        out_specs=(cells, vectors, P()),
        check_vma=False,
    )
```

```python
import math

import jax
import jax.numpy as jnp
from jax import lax
from jax.experimental import pallas as pl
from jax.experimental.pallas import tpu as pltpu
from jax.sharding import Mesh
from jax.sharding import PartitionSpec as P

ITERS = 2
GROUP = ("gx1", "gy", "gz")
F32 = jnp.float32
BF16 = jnp.bfloat16

kernel_var = 0.25
time_step = 2.0
particle_mass = 1.0 / 45.0
rest_density = 1.0
relaxation = 0.5
floor_value = 0.1
gravity = 0.1

KAPPA = math.log2(math.e) / kernel_var
YSCALE = math.sqrt(2.0 * KAPPA)
GRAD = 2.0 / kernel_var
ABSENT = 30000.0
PADDED = ((-1, 1), (0, 0), (0, 1), (1, 0))
VMEM = pl.BlockSpec(memory_space=pltpu.VMEM)
SMEM = pl.BlockSpec(memory_space=pltpu.SMEM)


def rows_iota(shape):
    return lax.broadcasted_iota(jnp.int32, shape, 0)


def split3(x):
    h = x.astype(BF16).astype(F32)
    m = (x - h).astype(BF16).astype(F32)
    return h, m, x - h - m


def stacked(x):
    h, m, l = split3(x)
    return jnp.concatenate([h, m, l, jnp.zeros_like(x)], 0).astype(BF16)


def unstacked(acc):
    return acc[0:8] + acc[8:16] + acc[16:24]


def dot(a, b):
    return jnp.dot(a, b, preferred_element_type=F32)


def plane_source(dy, dz):
    ny, nz = lax.axis_size("gy"), lax.axis_size("gz")
    y, z = lax.axis_index("gy"), lax.axis_index("gz")
    ok = (y + dy >= 0) & (y + dy < ny) & (z + dz >= 0) & (z + dz < nz)
    return jnp.where(ok, (y + dy) * nz + z + dz, y * nz + z), ok


def plane_start(other):
    g = lax.axis_index("gx1")
    return (1 - g if other else g) * (lax.axis_size("gy") * lax.axis_size("gz"))


def outer_x(x):
    g = lax.axis_index("gx1")
    return g if x == 0 else 1 - g


def pack_kernel(count, pos, vel, heading, cell, send, one):
    lane = lax.broadcasted_iota(jnp.int32, (1, 128), 1)
    code = jnp.where(lane < count[0, 0, 0], heading[0, 0] * 8 + cell[0, 0] + 1, 0).astype(F32)
    one[0:1, :] = code
    for f in range(3):
        one[1 + f : 2 + f, :] = pos[f, 0, 0]
        one[4 + f : 5 + f, :] = vel[f, 0, 0]
    one[7:8, :] = jnp.zeros((1, 128), F32)
    tile = one[...]
    for p in range(send.shape[0]):
        send[p] = tile


def prepare_kernel(pos, vel, pprev, counts, base, before, filled):
    lane2 = lax.broadcasted_iota(jnp.int32, (1, 2), 1)
    for c in range(8):
        x, y, z = outer_x(c // 4), c // 2 % 2, c % 2
        base[c, 0:1, :] = jnp.zeros((1, 128), F32)
        base[c, 7:8, :] = jnp.zeros((1, 128), F32)
        for f in range(3):
            base[c, 1 + f : 2 + f, :] = pos[f, x, y, z : z + 1, :]
            base[c, 4 + f : 5 + f, :] = vel[f, x, y, z : z + 1, :]
        before[c : c + 1, :] = pprev[x, y, z : z + 1, :]
        pair = counts[x, y : y + 1, :].astype(F32)
        count = jnp.sum(jnp.where(lane2 == z, pair, 0.0), 1, keepdims=True)
        filled[c : c + 1, :] = jnp.broadcast_to(count, (1, 128))


def fill_chunks(send, cell_of, rows):
    def put(p, cells):
        for k, c in enumerate(cells):
            if rows:
                send[p, k] = cell_of(c)
            else:
                send[p, k : k + 1, :] = cell_of(c)

    for p in range(send.shape[0]):
        put(p, range(4, 8))
    here = plane_start(False)
    for dy in (-1, 0, 1):
        for dz in (-1, 0, 1):
            if dy or dz:
                src, _ = plane_source(dy, dz)
                face = max(dz if dz else dy, 0)
                cells = [x * 4 + (k * 2 + face if dz else face * 2 + k) for x in range(2) for k in range(2)]
                put(here + src, cells)


def gather_kernel(recv, mine, l1, l2, near, far=None):
    here, there = plane_start(False), plane_start(True)
    whole = len(mine.shape) == 3

    def read(ref, p, k):
        return ref[p, k] if whole else ref[p, k : k + 1, :]

    for yp, (dy, y) in enumerate(PADDED):
        for zp, (dz, z) in enumerate(PADDED):
            src, ok = plane_source(dy, dz)
            q = yp * 4 + zp
            outs = [(near, jnp.where(ok, read(recv, there + src, y * 2 + z), 0.0))]
            if far is not None:
                outs.append((far, jnp.where(ok, read(recv, there + src, 4 + y * 2 + z), 0.0)))
            for x, out in enumerate((l1, l2)):
                if dy == 0 and dz == 0:
                    c = x * 4 + y * 2 + z
                    value = mine[c] if whole else mine[c : c + 1, :]
                else:
                    value = jnp.where(ok, read(recv, here + src, x * 2 + (y if dz else z)), 0.0)
                outs.append((out, value))
            for out, value in outs:
                if whole:
                    out[q] = value
                else:
                    out[q : q + 1, :] = value


def gather_last_kernel(recv, mine, send, l1, l2, near, far):
    gather_kernel(recv, mine, l1, l2, near, far)
    totals = recv[0, 8:16, :]
    for p in range(1, recv.shape[0]):
        totals = totals + recv[p, 8:16, :]
    layer = far[...]
    for p in range(send.shape[0]):
        send[p, 0:16, :] = layer
        send[p, 16:24, :] = totals


def insert_kernel(recv, beyond, base, counts, send, state):
    row = rows_iota((8, 128))
    lanef = lax.broadcasted_iota(jnp.int32, (8, 128), 1).astype(F32)
    here, there = plane_start(False), plane_start(True)
    g = lax.axis_index("gx1")
    cell = row + 4 * g - jnp.where(row >= 4, 8 * g, 0)
    cargos, marks = [], []
    for d in range(6):
        step = -1 if d % 2 == 0 else 1
        if d < 2:
            src, ok = plane_source(0, 0)
            tile = jnp.where(g == d, beyond[...], recv[there + src])
        else:
            src, ok = plane_source(step if d < 4 else 0, step if d >= 4 else 0)
            tile = recv[here + src]
        mark = (tile[0:1] == (cell + (d * 8 + 1)).astype(F32)) & ok
        cargos.append(stacked(tile))
        marks.append(jnp.where(mark, 1.0, 0.0))
    marked = jnp.concatenate(marks, 0).astype(BF16)
    r128 = rows_iota((128, 128))
    c128 = lax.broadcasted_iota(jnp.int32, (128, 128), 1)
    earlier = dot(marked, jnp.where(r128 < c128, 1.0, 0.0).astype(BF16))
    total = dot(marked, jnp.ones((128, 128), BF16))
    filled = counts[...]
    grown = filled
    targets = []
    for d in range(6):
        targets.append(jnp.where(marks[d] > 0, earlier[d * 8 : d * 8 + 8] + grown, -1.0))
        grown = grown + total[d * 8 : d * 8 + 8]
    slot = r128.astype(F32)
    for c in range(8):
        acc = jnp.zeros((32, 128), F32)
        for d in range(6):
            hot = jnp.where(slot == targets[d][c : c + 1], 1.0, 0.0).astype(BF16)
            acc = acc + lax.dot_general(
                cargos[d], hot, (((1,), (1,)), ((), ())), preferred_element_type=F32
            )
        tile = jnp.where(lanef < filled[c : c + 1], base[c], unstacked(acc))
        occ = lanef < grown[c : c + 1]
        tile = jnp.where(row == 0, 1.0, jnp.where(row == 7, 0.0, tile))
        state[c] = jnp.where(occ, tile, 0.0)
    fill_chunks(send, lambda c: state[c], True)


def column_features(xy, z, tile, xs, ys, xr, at, ft):
    row = rows_iota((8, 128))
    axis_row = (row >= 1) & (row <= 3)
    occ = tile[0:1]
    shift = jnp.where(row == 1, xs, jnp.where(row == 2, ys, jnp.where(row == 3, z - 2.0, 0.0)))
    st = (tile + shift) * occ
    xr[xy * 4 + z] = jnp.where(row < 4, st, 0.0)
    vx = jnp.sum(jnp.where(axis_row, st * pltpu.roll(st, 5, 0), 0.0), 0, keepdims=True)
    ft[xy, :, z * 128 : z * 128 + 128] = stacked(jnp.where(row == 7, vx, st))
    y = jnp.where(axis_row, st * YSCALE, 0.0)
    h, m, l = split3(y)
    qh, qm, ql = split3(jnp.where(occ > 0, 0.5 * jnp.sum(y * y, 0, keepdims=True), ABSENT))
    ones_rows = jnp.where((row >= 3) & (row < 6), 1.0, 0.0)
    qcol = jnp.where(row == 0, qh, jnp.where(row == 1, qm, jnp.where(row == 2, ql, ones_rows)))
    side = jnp.concatenate([h, h, m, m, h, l, qcol, jnp.zeros((8, 128), F32)], 0)
    at[xy, z * 128 : z * 128 + 128, :] = side.T.astype(BF16)
    return st


def centre_side(st):
    row = rows_iota((8, 128))
    y = jnp.where((row >= 1) & (row <= 3), st * YSCALE, 0.0)
    h, m, l = split3(y)
    qh, qm, ql = split3(0.5 * jnp.sum(y * y, 0, keepdims=True))
    minus_rows = jnp.where(row < 3, -1.0, 0.0)
    qrow = jnp.where(row == 3, -qh, jnp.where(row == 4, -qm, jnp.where(row == 5, -ql, minus_rows)))
    return jnp.concatenate([h, m, h, m, l, h, qrow, jnp.zeros((8, 128), F32)], 0).astype(BF16)


def weigh(side, b, put):
    inner = dot(side(128, 384), b)
    pieces = (
        (0, 0, dot(side(0, 128), b[:, 0:128])),
        (0, 128, inner[:, 0:128]),
        (1, 0, inner[:, 128:256]),
        (1, 256, dot(side(384, 512), b[:, 128:256])),
    )
    sums = [[jnp.zeros((8, 128), F32)] * 2 for _ in range(2)]
    for cz, k, e in pieces:
        w = jnp.exp2(e)
        hi = w.astype(BF16)
        put(cz, k, k + e.shape[0], hi, (w - hi.astype(F32)).astype(BF16))
        n = e.shape[0] // 8
        sums[cz] = [
            sums[cz][0] + jnp.sum(w.reshape(n, 8, 128), 0),
            sums[cz][1] + jnp.sum((w * w * e).reshape(n, 8, 128), 0),
        ]
    return sums


def main_columns(cx):
    if cx == 0:
        return [(k, k // 3, k % 3) for k in range(6)]
    return [(6 + k, k // 3, k % 3) for k in range(9)]


def setup_main_kernel(l1, l2, near, whi, wlo, xr, own, bside, ft, dpart, gpart, at, bi):
    g = lax.axis_index("gx1")
    for x, ref in enumerate((l1, l2, near)):
        xs = jnp.where(g == 0, x - 1.0, -1.0 * x)

        def column(y, carry, x=x, ref=ref, xs=xs):
            for z in range(4):
                column_features(x * 4 + y, z, ref[y * 4 + z], xs, (y - 2).astype(F32), xr, at, ft)
            return carry

        lax.fori_loop(0, 4, column, 0)
    row = rows_iota((8, 128))
    for c in range(8):
        cx, cy, cz = c // 4, c // 2 % 2, c % 2
        tile = (l1, l2)[cx][(cy + 1) * 4 + cz + 1]
        xs = jnp.where(g == 0, cx - 1.0, -1.0 * cx)
        shift = jnp.where(row == 1, xs, jnp.where(row == 2, cy - 1.0, jnp.where(row == 3, cz - 1.0, 0.0)))
        st = (tile + shift) * tile[0:1]
        own[c] = st
        bi[c // 2, :, cz * 128 : cz * 128 + 128] = centre_side(st)
    bside[...] = bi[0:2]

    def weights(cy, carry):
        for cx in range(2):
            b = bi[cx * 2 + cy]
            sums = [[jnp.zeros((8, 128), F32)] * 2 for _ in range(2)]
            for k, x, y in main_columns(cx):
                xy = x * 4 + cy + y

                def put(cz, lo, hi, a, b, k=k):
                    whi[cy, cz, k, lo:hi, :] = a
                    wlo[cy, cz, k, lo:hi, :] = b

                more = weigh(lambda lo, hi, xy=xy: at[xy, lo:hi, :], b, put)
                sums = [[p + q for p, q in zip(a, b)] for a, b in zip(sums, more)]
            for cz in range(2):
                dpart[(cx * 2 + cy) * 2 + cz], gpart[(cx * 2 + cy) * 2 + cz] = sums[cz]
        return carry

    lax.fori_loop(0, 2, weights, 0)


def unstacked_groups(acc):
    return [unstacked(acc[k : k + 32]) for k in range(0, acc.shape[0], 32)]


def slices(fts, column, cz):
    parts = [ft[column, :, cz * 128 : cz * 128 + 384] for ft in fts]
    return parts[0] if len(parts) == 1 else jnp.concatenate(parts, 0)


def main_pass(whi, wlo, fts, part):
    def centre(cy, carry):
        for cx in range(2):
            for cz in range(2):
                acc = jnp.zeros((32 * len(fts), 128), F32)
                for k, x, y in main_columns(cx):
                    f = slices(fts, x * 4 + cy + y, cz)
                    acc = acc + dot(f, whi[cy, cz, k]) + dot(f, wlo[cy, cz, k])
                for g, r in enumerate(unstacked_groups(acc)):
                    part[(cx * 2 + cy) * 2 + cz, g * 8 : g * 8 + 8, :] = r
        return carry

    lax.fori_loop(0, 2, centre, 0)


def beyond_pass(whi, wlo, fts, part, finish):
    for c in range(8):
        cx, cy, cz = c // 4, c // 2 % 2, c % 2
        r = [part[c, g * 8 : g * 8 + 8, :] for g in range(len(fts))]
        if cx == 0:
            acc = jnp.zeros((32 * len(fts), 128), F32)
            for y in range(3):
                f = slices(fts, cy + y, cz)
                acc = acc + dot(f, whi[cy, cz, y]) + dot(f, wlo[cy, cz, y])
            r = [p + q for p, q in zip(r, unstacked_groups(acc))]
        finish(c, *r)


def setup_beyond_kernel(beyond, own, bside, dpart, gpart, counts, pprev, whi, wlo, xr, ft, gsq, safe2, press, send, srow, at, dsum):
    g = lax.axis_index("gx1")
    xs = jnp.where(g == 0, -2.0, 1.0)
    for y in range(4):
        for z in range(4):
            column_features(y, z, beyond[y * 4 + z], xs, y - 2.0, xr, at, ft)
    gsq[...] = gpart[...]
    dsum[...] = dpart[...]
    for cy in range(2):
        for y in range(3):

            def put(cz, lo, hi, a, b, cy=cy, y=y):
                whi[cy, cz, y, lo:hi, :] = a
                wlo[cy, cz, y, lo:hi, :] = b

            more = weigh(lambda lo, hi, xy=cy + y: at[xy, lo:hi, :], bside[cy], put)
            for cz in range(2):
                c = cy * 2 + cz
                dsum[c] = dsum[c] + more[cz][0]
                gsq[c] = gsq[c] + more[cz][1]
    lane = lax.broadcasted_iota(jnp.int32, (1, 128), 1).astype(F32)
    for c in range(8):
        occ = own[c, 0:1, :] > 0
        safe = jnp.where(occ, particle_mass * jnp.sum(dsum[c], 0, keepdims=True), 1.0)
        pressure = jnp.where(lane < counts[c : c + 1, :], pprev[c : c + 1, :], 0.0)
        safe2[c : c + 1, :] = safe * safe
        press[c : c + 1, :] = pressure
        srow[c : c + 1, :] = jnp.where(occ, pressure / (safe * safe), 0.0)
    fill_chunks(send, lambda c: srow[c : c + 1, :], False)


def sources(st, r, gsq, safe2):
    row = rows_iota((8, 128))
    axis_row = (row >= 1) & (row <= 3)
    occ = st[0:1] > 0
    s0 = r[0:1]
    gr = jnp.where(axis_row, st * s0 - r, 0.0)
    density = particle_mass * s0
    pair = pltpu.roll(st, 5, 0) * gr - st * pltpu.roll(r, 5, 0)
    divergence = (-GRAD * particle_mass) * (
        jnp.sum(jnp.where(axis_row, pair, 0.0), 0, keepdims=True) + r[7:8]
    )
    grad_norm = (GRAD * particle_mass) ** 2 * jnp.sum(gr * gr, 0, keepdims=True)
    grad_square = (-GRAD * GRAD * particle_mass / KAPPA) * jnp.sum(gsq, 0, keepdims=True)
    source = jnp.where(occ, rest_density - (density + time_step * divergence), 0.0)
    weight = jnp.where(occ, particle_mass, 0.0)
    diagonal = jnp.maximum(
        time_step * time_step * (grad_norm + weight * grad_square) / safe2, floor_value
    )
    return gr, source, diagonal


def scaled_features(layer, base, xr, ft):
    for y in range(4):
        for z in range(4):
            q = y * 4 + z
            ft[base // 4 + y, :, z * 128 : z * 128 + 128] = stacked(layer[q : q + 1, :] * xr[base + q])


def accel_features(layer, base, xr, ft):
    row = rows_iota((8, 128))
    axis_row = (row >= 1) & (row <= 3)
    zeros4 = jnp.zeros((4, 128), F32)
    for y in range(4):
        for z in range(4):
            q = y * 4 + z
            a = jnp.concatenate([layer[q], zeros4], 0)
            ax = jnp.sum(jnp.where(axis_row, a * xr[base + q], 0.0), 0, keepdims=True)
            ft[base // 4 + y, :, z * 128 : z * 128 + 128] = stacked(jnp.where(row == 0, ax, a))


def main_kernel(l1, l2, near, xr, whi, wlo, part, ft, *, features):
    for x, layer in enumerate((l1, l2, near)):
        features(layer, x * 16, xr, ft)
    main_pass(whi, wlo, (ft,), part)


def first_main_kernel(l1, l2, near, xr, whi, wlo, fs, part, ft):
    for x, layer in enumerate((l1, l2, near)):
        scaled_features(layer, x * 16, xr, ft)
    main_pass(whi, wlo, (fs, ft), part)


def own_row(c):
    return (c // 2 % 2 + 1) * 4 + c % 2 + 1


def accel_of(c, r, l1, l2, xr, grad):
    q = own_row(c)
    s = (l1, l2)[c // 4][q : q + 1, :]
    return (GRAD * particle_mass) * (s * grad + xr[c // 4 * 16 + q] * r[0:1] - r)


def accel_kernel(beyond, xrb, whi, wlo, part, l1, l2, xr, grad, send, mine, ft):
    scaled_features(beyond, 0, xrb, ft)

    def finish(c, r):
        mine[c] = accel_of(c, r, l1, l2, xr, grad[c])[0:4]

    beyond_pass(whi, wlo, (ft,), part, finish)
    fill_chunks(send, lambda c: mine[c], True)


def first_accel_kernel(beyond, xrb, whi, wlo, fs, part, l1, l2, xr, own, gsq, safe2, send, mine, grad, aux, ft):
    scaled_features(beyond, 0, xrb, ft)

    def finish(c, rs, r):
        squared = safe2[c : c + 1, :]
        gr, source, diagonal = sources(own[c], rs, gsq[c], squared)
        grad[c] = gr
        aux[c, 0:1, :] = squared
        aux[c, 1:2, :] = source
        aux[c, 2:3, :] = diagonal
        mine[c] = accel_of(c, r, l1, l2, xr, gr)[0:4]

    beyond_pass(whi, wlo, (fs, ft), part, finish)
    fill_chunks(send, lambda c: mine[c], True)


def apply_kernel(beyond, xrb, whi, wlo, part, l1, l2, xr, grad, aux, press, errs, pnew, enew, send, mine, ft, *, at_iter, last):
    row = rows_iota((8, 128))
    axis_row = (row >= 1) & (row <= 3)
    zeros4 = jnp.zeros((4, 128), F32)
    accel_features(beyond, 0, xrb, ft)
    enew[...] = jnp.zeros((8, 128), F32) if errs is None else errs[...]

    def finish(c, r):
        q = own_row(c)
        a = jnp.concatenate([(l1, l2)[c // 4][q], zeros4], 0)
        x = xr[c // 4 * 16 + q]
        inner = jnp.sum(jnp.where(axis_row, a * grad[c] - x * r, 0.0), 0, keepdims=True) + r[0:1]
        applied = (-time_step * time_step * GRAD * particle_mass) * inner
        occ = x[0:1] > 0
        safe2, source, diagonal = (aux[c, k : k + 1, :] for k in range(3))
        residual = jnp.where(occ, source - applied, 0.0)
        enew[at_iter : at_iter + 1, :] = enew[at_iter : at_iter + 1, :] + jnp.abs(residual)
        p = press[c : c + 1, :]
        p = jnp.where(occ, jnp.maximum(p + relaxation * (applied - source) / diagonal, 0.0), 0.0)
        if last:
            pnew[outer_x(c // 4), c // 2 % 2, c % 2 : c % 2 + 1, :] = p
        else:
            pnew[c : c + 1, :] = p
        mine[c : c + 1, :] = jnp.where(occ, p / safe2, 0.0)

    beyond_pass(whi, wlo, (ft,), part, finish)
    fill_chunks(send, lambda c: mine[c : c + 1, :], False)
    if last:
        first, totals = mine[0:4, :], enew[...]
        for p in range(send.shape[0]):
            send[p, 4:8, :] = first
            send[p, 8:16, :] = totals


def final_kernel(recv, xrb, whi, wlo, part, l1, l2, xr, grad, state, vout, eout, beyond, ft, *, slots):
    n = recv.shape[0]
    totals = recv[0, 16:24, :]
    for p in range(1, n):
        totals = totals + recv[p, 16:24, :]
    for it in range(ITERS):
        eout[it] = jnp.sum(totals[it : it + 1, :]) / slots
    src = lax.axis_index("gx0") + 2 * lax.axis_index("gx1") - 1
    ok = (src >= 0) & (src < n)
    beyond[...] = jnp.where(ok, recv[jnp.where(ok, src, 0), 0:16, :], 0.0)
    scaled_features(beyond, 0, xrb, ft)
    row = rows_iota((8, 128))

    def finish(c, r):
        a = accel_of(c, r, l1, l2, xr, grad[c])
        st = state[c]
        pulled = a - jnp.where(row == 3, gravity, 0.0)
        v = pltpu.roll(st, 5, 0) + time_step * pulled
        v = jnp.where(st[0:1] > 0, v, 0.0)
        for f in range(3):
            vout[f, outer_x(c // 4), c // 2 % 2, c % 2 : c % 2 + 1, :] = v[1 + f : 2 + f]

    beyond_pass(whi, wlo, (ft,), part, finish)


def call(body, outs, operands, scratch=(), limit=12 << 20, flops=0, first=None, **static):
    def named(*refs):
        body(*refs, **static)

    specs = [VMEM] * len(operands)
    if first is not None:
        specs[0] = first
    return pl.pallas_call(
        named,
        out_shape=outs,
        in_specs=specs,
        out_specs=jax.tree.map(lambda o: SMEM if o.shape == (ITERS,) else VMEM, outs),
        scratch_shapes=list(scratch),
        compiler_params=pltpu.CompilerParams(vmem_limit_bytes=limit),
        cost_estimate=pl.CostEstimate(flops=flops, transcendentals=0, bytes_accessed=0) if flops else None,
    )(*operands)


def sds(*shape, dtype=F32):
    return jax.ShapeDtypeStruct(shape, dtype)


def on_device(positions, velocities, pressure_prev, counts, out_positions, out_velocities, out_dir, out_cell, out_count):
    pairs, plane = lax.axis_size("gx0"), lax.axis_size("gy") * lax.axis_size("gz")
    group = 2 * plane
    across = [(2 * j + 1, 2 * j + 2) for j in range(pairs - 1)]
    across = across + [(b, a) for a, b in across]
    busy = 4 * 10**9

    def spread(send):
        return lax.all_to_all(send, GROUP, 0, 0)

    def from_beyond(layer):
        return lax.ppermute(layer, ("gx0", "gx1"), across)

    def layers(send, mine, shape):
        return call(gather_kernel, (sds(16, *shape),) * 3, (spread(send), mine))

    def features(columns):
        return pltpu.VMEM((columns, 32, 512), BF16)

    tiles, rows = sds(8, 8, 128), sds(8, 128)
    send, one = call(
        pack_kernel,
        (sds(group, 8, 128), rows),
        (out_count, out_positions, out_velocities, out_dir, out_cell),
        limit=60 * 1024 * 1024,
        first=SMEM,
    )
    base, before, filled = call(
        prepare_kernel, (tiles, rows, rows), (positions, velocities, pressure_prev, counts), flops=busy // 4
    )
    send, state = call(insert_kernel, (sds(group, 4, 8, 128), tiles), (spread(send), from_beyond(one), base, filled))
    l1, l2, near = layers(send, state, (8, 128))
    beyond = from_beyond(l1)
    wmain, wside = sds(2, 2, 15, 384, 128, dtype=BF16), sds(2, 2, 3, 384, 128, dtype=BF16)
    fshape = sds(12, 32, 512, dtype=BF16)
    whi, wlo, xr, own, bside, fs, dpart, gpart = call(
        setup_main_kernel,
        (wmain, wmain, sds(48, 8, 128), tiles, sds(2, 64, 256, dtype=BF16), fshape, tiles, tiles),
        (l1, l2, near),
        [pltpu.VMEM((12, 512, 64), BF16), pltpu.VMEM((4, 64, 256), BF16)],
        flops=3 * busy,
    )
    bhi, blo, xrb, fsb, gsq, safe2, press, send, mine = call(
        setup_beyond_kernel,
        (wside, wside, sds(16, 8, 128), sds(4, 32, 512, dtype=BF16), tiles, rows, rows, sds(group, 4, 128), rows),
        (beyond, own, bside, dpart, gpart, filled, before),
        [pltpu.VMEM((4, 512, 64), BF16), pltpu.VMEM((8, 8, 128), F32)],
    )
    errs = None
    for it in range(ITERS):
        last = it == ITERS - 1
        l1, l2, near = layers(send, mine, (128,))
        beyond = from_beyond(l1)
        accels = (sds(group, 4, 4, 128), sds(8, 4, 128))
        if it == 0:
            (part,) = call(
                first_main_kernel, (sds(8, 16, 128),), (l1, l2, near, xr, whi, wlo, fs), [features(12)], flops=busy
            )
            send, mine, grad, aux = call(
                first_accel_kernel,
                (*accels, tiles, tiles),
                (beyond, xrb, bhi, blo, fsb, part, l1, l2, xr, own, gsq, safe2),
                [features(4)],
            )
        else:
            (part,) = call(
                main_kernel, (tiles,), (l1, l2, near, xr, whi, wlo), [features(12)], flops=busy, features=scaled_features
            )
            send, mine = call(
                accel_kernel, accels, (beyond, xrb, bhi, blo, part, l1, l2, xr, grad), [features(4)]
            )
        l1, l2, near = layers(send, mine, (4, 128))
        beyond = from_beyond(l1)
        (part,) = call(
            main_kernel, (tiles,), (l1, l2, near, xr, whi, wlo), [features(12)], flops=busy, features=accel_features
        )

        def body(*refs, it=it, last=last):
            refs = refs if it else (*refs[:11], None, *refs[11:])
            apply_kernel(*refs, at_iter=it, last=last)

        operands = (beyond, xrb, bhi, blo, part, l1, l2, xr, grad, aux, press) + (() if it == 0 else (errs,))
        press, errs, send, mine = call(
            body,
            (sds(2, 2, 2, 128) if last else rows, rows, sds(group, 16 if last else 4, 128), rows),
            operands,
            [features(4)],
        )
    send, l1, l2, near, _ = call(
        gather_last_kernel, (sds(pairs, 24, 128),) + (sds(16, 128),) * 4, (spread(send), mine)
    )
    recv = lax.all_to_all(send, "gx0", 0, 0)
    (part,) = call(
        main_kernel, (tiles,), (l1, l2, near, xr, whi, wlo), [features(12)], flops=busy, features=scaled_features
    )
    velocity_new, density_error = call(
        final_kernel,
        (sds(3, 2, 2, 2, 128), sds(ITERS)),
        (recv, xrb, bhi, blo, part, l1, l2, xr, grad, state),
        [pltpu.VMEM((16, 128), F32), features(4)],
        slots=pairs * group * 8 * 128,
    )
    return press, velocity_new, density_error


def solution(mesh):
    nx, ny, nz = (mesh.shape[a] for a in ("gx", "gy", "gz"))
    paired = Mesh(mesh.devices.reshape(nx // 2, 2, ny, nz), ("gx0", "gx1", "gy", "gz"))
    gx = ("gx0", "gx1")
    cells = P(gx, "gy", "gz", None)
    vectors = P(None, gx, "gy", "gz", None)
    ints = P(gx, "gy", "gz")
    return jax.shard_map(
        on_device,
        mesh=paired,
        in_specs=(vectors, vectors, cells, ints, vectors, vectors, cells, cells, ints),
        out_specs=(cells, vectors, P()),
        check_vma=False,
    )
```

```python
import math

import jax
import jax.numpy as jnp
from jax import lax
from jax.experimental import pallas as pl
from jax.experimental.pallas import tpu as pltpu
from jax.sharding import Mesh
from jax.sharding import PartitionSpec as P

ITERS = 2
GROUP = ("gx1", "gy", "gz")
F32 = jnp.float32
BF16 = jnp.bfloat16

kernel_var = 0.25
time_step = 2.0
particle_mass = 1.0 / 45.0
rest_density = 1.0
relaxation = 0.5
floor_value = 0.1
gravity = 0.1

KAPPA = math.log2(math.e) / kernel_var
YSCALE = math.sqrt(2.0 * KAPPA)
GRAD = 2.0 / kernel_var
ABSENT = 30000.0
PADDED = ((-1, 1), (0, 0), (0, 1), (1, 0))
VMEM = pl.BlockSpec(memory_space=pltpu.VMEM)
SMEM = pl.BlockSpec(memory_space=pltpu.SMEM)


def rows_iota(shape):
    return lax.broadcasted_iota(jnp.int32, shape, 0)


def split3(x):
    h = x.astype(BF16).astype(F32)
    m = (x - h).astype(BF16).astype(F32)
    return h, m, x - h - m


def stacked(x):
    h, m, l = split3(x)
    return jnp.concatenate([h, m, l, jnp.zeros_like(x)], 0).astype(BF16)


def unstacked(acc):
    return acc[0:8] + acc[8:16] + acc[16:24]


def dot(a, b):
    return jnp.dot(a, b, preferred_element_type=F32)


def plane_source(dy, dz):
    ny, nz = lax.axis_size("gy"), lax.axis_size("gz")
    y, z = lax.axis_index("gy"), lax.axis_index("gz")
    ok = (y + dy >= 0) & (y + dy < ny) & (z + dz >= 0) & (z + dz < nz)
    return jnp.where(ok, (y + dy) * nz + z + dz, y * nz + z), ok


def plane_start(other):
    g = lax.axis_index("gx1")
    return (1 - g if other else g) * (lax.axis_size("gy") * lax.axis_size("gz"))


def outer_x(x):
    g = lax.axis_index("gx1")
    return g if x == 0 else 1 - g


def pack_kernel(count, pos, vel, heading, cell, send, one):
    lane = lax.broadcasted_iota(jnp.int32, (1, 128), 1)
    code = jnp.where(lane < count[0, 0, 0], heading[0, 0] * 8 + cell[0, 0] + 1, 0).astype(F32)
    one[0:1, :] = code
    for f in range(3):
        one[1 + f : 2 + f, :] = pos[f, 0, 0]
        one[4 + f : 5 + f, :] = vel[f, 0, 0]
    one[7:8, :] = jnp.zeros((1, 128), F32)
    tile = one[...]
    for p in range(send.shape[0]):
        send[p] = tile


def prepare_kernel(pos, vel, pprev, counts, base, before, filled):
    lane2 = lax.broadcasted_iota(jnp.int32, (1, 2), 1)
    for c in range(8):
        x, y, z = outer_x(c // 4), c // 2 % 2, c % 2
        base[c, 0:1, :] = jnp.zeros((1, 128), F32)
        base[c, 7:8, :] = jnp.zeros((1, 128), F32)
        for f in range(3):
            base[c, 1 + f : 2 + f, :] = pos[f, x, y, z : z + 1, :]
            base[c, 4 + f : 5 + f, :] = vel[f, x, y, z : z + 1, :]
        before[c : c + 1, :] = pprev[x, y, z : z + 1, :]
        pair = counts[x, y : y + 1, :].astype(F32)
        count = jnp.sum(jnp.where(lane2 == z, pair, 0.0), 1, keepdims=True)
        filled[c : c + 1, :] = jnp.broadcast_to(count, (1, 128))


def fill_chunks(send, cell_of, rows):
    def put(p, cells):
        for k, c in enumerate(cells):
            if rows:
                send[p, k] = cell_of(c)
            else:
                send[p, k : k + 1, :] = cell_of(c)

    for p in range(send.shape[0]):
        put(p, range(4, 8))
    here = plane_start(False)
    for dy in (-1, 0, 1):
        for dz in (-1, 0, 1):
            if dy or dz:
                src, _ = plane_source(dy, dz)
                face = max(dz if dz else dy, 0)
                cells = [x * 4 + (k * 2 + face if dz else face * 2 + k) for x in range(2) for k in range(2)]
                put(here + src, cells)


def gather_kernel(recv, mine, l1, l2, near, far=None):
    here, there = plane_start(False), plane_start(True)
    whole = len(mine.shape) == 3

    def read(ref, p, k):
        return ref[p, k] if whole else ref[p, k : k + 1, :]

    for yp, (dy, y) in enumerate(PADDED):
        for zp, (dz, z) in enumerate(PADDED):
            src, ok = plane_source(dy, dz)
            q = yp * 4 + zp
            outs = [(near, jnp.where(ok, read(recv, there + src, y * 2 + z), 0.0))]
            if far is not None:
                outs.append((far, jnp.where(ok, read(recv, there + src, 4 + y * 2 + z), 0.0)))
            for x, out in enumerate((l1, l2)):
                if dy == 0 and dz == 0:
                    c = x * 4 + y * 2 + z
                    value = mine[c] if whole else mine[c : c + 1, :]
                else:
                    value = jnp.where(ok, read(recv, here + src, x * 2 + (y if dz else z)), 0.0)
                outs.append((out, value))
            for out, value in outs:
                if whole:
                    out[q] = value
                else:
                    out[q : q + 1, :] = value


def gather_last_kernel(recv, mine, send, l1, l2, near, far):
    gather_kernel(recv, mine, l1, l2, near, far)
    totals = recv[0, 8:16, :]
    for p in range(1, recv.shape[0]):
        totals = totals + recv[p, 8:16, :]
    layer = far[...]
    for p in range(send.shape[0]):
        send[p, 0:16, :] = layer
        send[p, 16:24, :] = totals


def insert_kernel(recv, beyond, base, counts, send, state, places):
    row = rows_iota((8, 128))
    lanef = lax.broadcasted_iota(jnp.int32, (8, 128), 1).astype(F32)
    here, there = plane_start(False), plane_start(True)
    g = lax.axis_index("gx1")
    cell = row + 4 * g - jnp.where(row >= 4, 8 * g, 0)
    cargos, marks = [], []
    for d in range(6):
        step = -1 if d % 2 == 0 else 1
        if d < 2:
            src, ok = plane_source(0, 0)
            tile = jnp.where(g == d, beyond[...], recv[there + src])
        else:
            src, ok = plane_source(step if d < 4 else 0, step if d >= 4 else 0)
            tile = recv[here + src]
        mark = (tile[0:1] == (cell + (d * 8 + 1)).astype(F32)) & ok
        cargos.append(stacked(tile))
        marks.append(jnp.where(mark, 1.0, 0.0))
    marked = jnp.concatenate(marks, 0).astype(BF16)
    r128 = rows_iota((128, 128))
    c128 = lax.broadcasted_iota(jnp.int32, (128, 128), 1)
    earlier = dot(marked, jnp.where(r128 < c128, 1.0, 0.0).astype(BF16))
    total = dot(marked, jnp.ones((128, 128), BF16))
    filled = counts[...]
    grown = filled
    targets = []
    for d in range(6):
        targets.append(jnp.where(marks[d] > 0, earlier[d * 8 : d * 8 + 8] + grown, -1.0))
        grown = grown + total[d * 8 : d * 8 + 8]
    slot = r128.astype(F32)
    for c in range(8):
        acc = jnp.zeros((32, 128), F32)
        for d in range(6):
            hot = jnp.where(slot == targets[d][c : c + 1], 1.0, 0.0).astype(BF16)
            acc = acc + lax.dot_general(
                cargos[d], hot, (((1,), (1,)), ((), ())), preferred_element_type=F32
            )
        tile = jnp.where(lanef < filled[c : c + 1], base[c], unstacked(acc))
        occ = lanef < grown[c : c + 1]
        tile = jnp.where(row == 0, 1.0, jnp.where(row == 7, 0.0, tile))
        tile = jnp.where(occ, tile, 0.0)
        state[c] = tile
        places[c] = tile[0:4]
    fill_chunks(send, lambda c: places[c], True)


def column_features(xy, z, place, xs, ys, xr, at):
    row = rows_iota((8, 128))
    axis_row = (row >= 1) & (row <= 3)
    tile = jnp.concatenate([place, jnp.zeros((4, 128), F32)], 0)
    occ = tile[0:1]
    shift = jnp.where(row == 1, xs, jnp.where(row == 2, ys, jnp.where(row == 3, z - 2.0, 0.0)))
    st = (tile + shift) * occ
    xr[xy * 4 + z] = st
    y = jnp.where(axis_row, st * YSCALE, 0.0)
    h, m, l = split3(y)
    qh, qm, ql = split3(jnp.where(occ > 0, 0.5 * jnp.sum(y * y, 0, keepdims=True), ABSENT))
    ones_rows = jnp.where((row >= 3) & (row < 6), 1.0, 0.0)
    qcol = jnp.where(row == 0, qh, jnp.where(row == 1, qm, jnp.where(row == 2, ql, ones_rows)))
    side = jnp.concatenate([h, h, m, m, h, l, qcol, jnp.zeros((8, 128), F32)], 0)
    at[xy, z * 128 : z * 128 + 128, :] = side.T.astype(BF16)
    return st


def centre_side(st):
    row = rows_iota((8, 128))
    y = jnp.where((row >= 1) & (row <= 3), st * YSCALE, 0.0)
    h, m, l = split3(y)
    qh, qm, ql = split3(0.5 * jnp.sum(y * y, 0, keepdims=True))
    minus_rows = jnp.where(row < 3, -1.0, 0.0)
    qrow = jnp.where(row == 3, -qh, jnp.where(row == 4, -qm, jnp.where(row == 5, -ql, minus_rows)))
    return jnp.concatenate([h, m, h, m, l, h, qrow, jnp.zeros((8, 128), F32)], 0).astype(BF16)


def weigh(side, b, put):
    inner = dot(side(128, 384), b)
    pieces = (
        (0, 0, dot(side(0, 128), b[:, 0:128])),
        (0, 128, inner[:, 0:128]),
        (1, 0, inner[:, 128:256]),
        (1, 256, dot(side(384, 512), b[:, 128:256])),
    )
    sums = [[jnp.zeros((8, 128), F32)] * 2 for _ in range(2)]
    for cz, k, e in pieces:
        w = jnp.exp2(e)
        hi = w.astype(BF16)
        put(cz, k, k + e.shape[0], hi, (w - hi.astype(F32)).astype(BF16))
        n = e.shape[0] // 8
        sums[cz] = [
            sums[cz][0] + jnp.sum(w.reshape(n, 8, 128), 0),
            sums[cz][1] + jnp.sum((w * w * e).reshape(n, 8, 128), 0),
        ]
    return sums


def main_columns(cx):
    if cx == 0:
        return [(k, k // 3, k % 3) for k in range(6)]
    return [(6 + k, k // 3, k % 3) for k in range(9)]


def setup_main_kernel(l1, l2, near, state, whi, wlo, xr, own, bside, dpart, gpart, at, bi):
    g = lax.axis_index("gx1")
    for x, ref in enumerate((l1, l2, near)):
        xs = jnp.where(g == 0, x - 1.0, -1.0 * x)

        def column(y, carry, x=x, ref=ref, xs=xs):
            for z in range(4):
                column_features(x * 4 + y, z, ref[y * 4 + z], xs, (y - 2).astype(F32), xr, at)
            return carry

        lax.fori_loop(0, 4, column, 0)
    row = rows_iota((8, 128))
    for c in range(8):
        cx, cy, cz = c // 4, c // 2 % 2, c % 2
        tile = state[c]
        xs = jnp.where(g == 0, cx - 1.0, -1.0 * cx)
        shift = jnp.where(row == 1, xs, jnp.where(row == 2, cy - 1.0, jnp.where(row == 3, cz - 1.0, 0.0)))
        st = (tile + shift) * tile[0:1]
        own[c] = st
        bi[c // 2, :, cz * 128 : cz * 128 + 128] = centre_side(st)
    bside[...] = bi[0:2]

    def weights(cy, carry):
        for cx in range(2):
            b = bi[cx * 2 + cy]
            sums = [[jnp.zeros((8, 128), F32)] * 2 for _ in range(2)]
            for k, x, y in main_columns(cx):
                xy = x * 4 + cy + y

                def put(cz, lo, hi, a, b, k=k):
                    whi[cy, cz, k, lo:hi, :] = a
                    wlo[cy, cz, k, lo:hi, :] = b

                more = weigh(lambda lo, hi, xy=xy: at[xy, lo:hi, :], b, put)
                sums = [[p + q for p, q in zip(a, b)] for a, b in zip(sums, more)]
            for cz in range(2):
                dpart[(cx * 2 + cy) * 2 + cz], gpart[(cx * 2 + cy) * 2 + cz] = sums[cz]
        return carry

    lax.fori_loop(0, 2, weights, 0)


def unstacked_groups(acc):
    return [unstacked(acc[k : k + 32]) for k in range(0, acc.shape[0], 32)]


def slices(fts, column, cz):
    parts = [ft[column, :, cz * 128 : cz * 128 + 384] for ft in fts]
    return parts[0] if len(parts) == 1 else jnp.concatenate(parts, 0)


def main_pass(whi, wlo, fts, part):
    def centre(cy, carry):
        for cx in range(2):
            for cz in range(2):
                acc = jnp.zeros((32 * len(fts), 128), F32)
                for k, x, y in main_columns(cx):
                    f = slices(fts, x * 4 + cy + y, cz)
                    acc = acc + dot(f, whi[cy, cz, k]) + dot(f, wlo[cy, cz, k])
                for g, r in enumerate(unstacked_groups(acc)):
                    part[(cx * 2 + cy) * 2 + cz, g * 8 : g * 8 + 8, :] = r
        return carry

    lax.fori_loop(0, 2, centre, 0)


def beyond_pass(whi, wlo, fts, part, finish):
    for c in range(8):
        cx, cy, cz = c // 4, c // 2 % 2, c % 2
        r = [part[c, g * 8 : g * 8 + 8, :] for g in range(len(fts))]
        if cx == 0:
            acc = jnp.zeros((32 * len(fts), 128), F32)
            for y in range(3):
                f = slices(fts, cy + y, cz)
                acc = acc + dot(f, whi[cy, cz, y]) + dot(f, wlo[cy, cz, y])
            r = [p + q for p, q in zip(r, unstacked_groups(acc))]
        finish(c, *r)


def setup_beyond_kernel(beyond, own, bside, dpart, gpart, counts, pprev, whi, wlo, xr, gsq, safe2, press, send, mine, at, dsum):
    g = lax.axis_index("gx1")
    xs = jnp.where(g == 0, -2.0, 1.0)
    for y in range(4):
        for z in range(4):
            column_features(y, z, beyond[y * 4 + z], xs, y - 2.0, xr, at)
    gsq[...] = gpart[...]
    dsum[...] = dpart[...]
    for cy in range(2):
        for y in range(3):

            def put(cz, lo, hi, a, b, cy=cy, y=y):
                whi[cy, cz, y, lo:hi, :] = a
                wlo[cy, cz, y, lo:hi, :] = b

            more = weigh(lambda lo, hi, xy=cy + y: at[xy, lo:hi, :], bside[cy], put)
            for cz in range(2):
                c = cy * 2 + cz
                dsum[c] = dsum[c] + more[cz][0]
                gsq[c] = gsq[c] + more[cz][1]
    lane = lax.broadcasted_iota(jnp.int32, (1, 128), 1).astype(F32)
    for c in range(8):
        occ = own[c, 0:1, :] > 0
        safe = jnp.where(occ, particle_mass * jnp.sum(dsum[c], 0, keepdims=True), 1.0)
        pressure = jnp.where(lane < counts[c : c + 1, :], pprev[c : c + 1, :], 0.0)
        safe2[c : c + 1, :] = safe * safe
        press[c : c + 1, :] = pressure
        mine[c, 0:1, :] = jnp.where(occ, pressure / (safe * safe), 0.0)
        mine[c, 1:4, :] = own[c, 4:7, :]
    fill_chunks(send, lambda c: mine[c], True)


def sources(st, r, gsq, safe2):
    row = rows_iota((8, 128))
    axis_row = (row >= 1) & (row <= 3)
    occ = st[0:1] > 0
    s0 = r[0:1]
    gr = jnp.where(axis_row, st * s0 - r, 0.0)
    density = particle_mass * s0
    pair = pltpu.roll(st, 5, 0) * gr - st * pltpu.roll(r, 5, 0)
    divergence = (-GRAD * particle_mass) * (
        jnp.sum(jnp.where(axis_row, pair, 0.0), 0, keepdims=True) + r[7:8]
    )
    grad_norm = (GRAD * particle_mass) ** 2 * jnp.sum(gr * gr, 0, keepdims=True)
    grad_square = (-GRAD * GRAD * particle_mass / KAPPA) * jnp.sum(gsq, 0, keepdims=True)
    source = jnp.where(occ, rest_density - (density + time_step * divergence), 0.0)
    weight = jnp.where(occ, particle_mass, 0.0)
    diagonal = jnp.maximum(
        time_step * time_step * (grad_norm + weight * grad_square) / safe2, floor_value
    )
    return gr, source, diagonal


def scaled_features(layer, base, xr, ft):
    for y in range(4):
        for z in range(4):
            q = y * 4 + z
            ft[base // 4 + y, :, z * 128 : z * 128 + 128] = stacked(layer[q : q + 1, :] * xr[base + q])


def first_features(layer, base, xr, fs, ft):
    row = rows_iota((8, 128))
    for y in range(4):
        for z in range(4):
            q = y * 4 + z
            x = xr[base + q]
            t = jnp.concatenate([layer[q], jnp.zeros((4, 128), F32)], 0)
            vx = jnp.sum(jnp.where((row >= 1) & (row <= 3), x * t, 0.0), 0, keepdims=True)
            v = jnp.where((row >= 4) & (row <= 6), pltpu.roll(t, 3, 0), 0.0)
            fs[base // 4 + y, :, z * 128 : z * 128 + 128] = stacked(jnp.where(row == 7, vx, x + v))
            ft[base // 4 + y, :, z * 128 : z * 128 + 128] = stacked(t[0:1] * x)


def accel_features(layer, base, xr, ft):
    row = rows_iota((8, 128))
    axis_row = (row >= 1) & (row <= 3)
    zeros4 = jnp.zeros((4, 128), F32)
    for y in range(4):
        for z in range(4):
            q = y * 4 + z
            a = jnp.concatenate([layer[q], zeros4], 0)
            ax = jnp.sum(jnp.where(axis_row, a * xr[base + q], 0.0), 0, keepdims=True)
            ft[base // 4 + y, :, z * 128 : z * 128 + 128] = stacked(jnp.where(row == 0, ax, a))


def main_kernel(l1, l2, near, xr, whi, wlo, part, ft, *, features):
    for x, layer in enumerate((l1, l2, near)):
        features(layer, x * 16, xr, ft)
    main_pass(whi, wlo, (ft,), part)


def first_main_kernel(l1, l2, near, xr, whi, wlo, part, fs, ft):
    for x, layer in enumerate((l1, l2, near)):
        first_features(layer, x * 16, xr, fs, ft)
    main_pass(whi, wlo, (fs, ft), part)


def own_row(c):
    return (c // 2 % 2 + 1) * 4 + c % 2 + 1


def accel_of(c, r, l1, l2, xr, grad):
    q = own_row(c)
    layer = (l1, l2)[c // 4]
    s = layer[q : q + 1, :] if len(layer.shape) == 2 else layer[q, 0:1, :]
    return (GRAD * particle_mass) * (s * grad + xr[c // 4 * 16 + q] * r[0:1] - r)


def accel_kernel(beyond, xrb, whi, wlo, part, l1, l2, xr, grad, send, mine, ft):
    scaled_features(beyond, 0, xrb, ft)

    def finish(c, r):
        mine[c] = accel_of(c, r, l1, l2, xr, grad[c])[0:4]

    beyond_pass(whi, wlo, (ft,), part, finish)
    fill_chunks(send, lambda c: mine[c], True)


def first_accel_kernel(beyond, xrb, whi, wlo, part, l1, l2, xr, own, gsq, safe2, send, mine, grad, aux, fs, ft):
    first_features(beyond, 0, xrb, fs, ft)

    def finish(c, rs, r):
        squared = safe2[c : c + 1, :]
        gr, source, diagonal = sources(own[c], rs, gsq[c], squared)
        grad[c] = gr
        aux[c, 0:1, :] = squared
        aux[c, 1:2, :] = source
        aux[c, 2:3, :] = diagonal
        mine[c] = accel_of(c, r, l1, l2, xr, gr)[0:4]

    beyond_pass(whi, wlo, (fs, ft), part, finish)
    fill_chunks(send, lambda c: mine[c], True)


def apply_kernel(beyond, xrb, whi, wlo, part, l1, l2, xr, grad, aux, press, errs, pnew, enew, send, mine, ft, *, at_iter, last):
    row = rows_iota((8, 128))
    axis_row = (row >= 1) & (row <= 3)
    zeros4 = jnp.zeros((4, 128), F32)
    accel_features(beyond, 0, xrb, ft)
    enew[...] = jnp.zeros((8, 128), F32) if errs is None else errs[...]

    def finish(c, r):
        q = own_row(c)
        a = jnp.concatenate([(l1, l2)[c // 4][q], zeros4], 0)
        x = xr[c // 4 * 16 + q]
        inner = jnp.sum(jnp.where(axis_row, a * grad[c] - x * r, 0.0), 0, keepdims=True) + r[0:1]
        applied = (-time_step * time_step * GRAD * particle_mass) * inner
        occ = x[0:1] > 0
        safe2, source, diagonal = (aux[c, k : k + 1, :] for k in range(3))
        residual = jnp.where(occ, source - applied, 0.0)
        enew[at_iter : at_iter + 1, :] = enew[at_iter : at_iter + 1, :] + jnp.abs(residual)
        p = press[c : c + 1, :]
        p = jnp.where(occ, jnp.maximum(p + relaxation * (applied - source) / diagonal, 0.0), 0.0)
        if last:
            pnew[outer_x(c // 4), c // 2 % 2, c % 2 : c % 2 + 1, :] = p
        else:
            pnew[c : c + 1, :] = p
        mine[c : c + 1, :] = jnp.where(occ, p / safe2, 0.0)

    beyond_pass(whi, wlo, (ft,), part, finish)
    fill_chunks(send, lambda c: mine[c : c + 1, :], False)
    if last:
        first, totals = mine[0:4, :], enew[...]
        for p in range(send.shape[0]):
            send[p, 4:8, :] = first
            send[p, 8:16, :] = totals


def final_kernel(recv, xrb, whi, wlo, part, l1, l2, xr, grad, state, vout, eout, beyond, ft, *, slots):
    n = recv.shape[0]
    totals = recv[0, 16:24, :]
    for p in range(1, n):
        totals = totals + recv[p, 16:24, :]
    for it in range(ITERS):
        eout[it] = jnp.sum(totals[it : it + 1, :]) / slots
    src = lax.axis_index("gx0") + 2 * lax.axis_index("gx1") - 1
    ok = (src >= 0) & (src < n)
    beyond[...] = jnp.where(ok, recv[jnp.where(ok, src, 0), 0:16, :], 0.0)
    scaled_features(beyond, 0, xrb, ft)
    row = rows_iota((8, 128))

    def finish(c, r):
        a = accel_of(c, r, l1, l2, xr, grad[c])
        st = state[c]
        pulled = a - jnp.where(row == 3, gravity, 0.0)
        v = pltpu.roll(st, 5, 0) + time_step * pulled
        v = jnp.where(st[0:1] > 0, v, 0.0)
        for f in range(3):
            vout[f, outer_x(c // 4), c // 2 % 2, c % 2 : c % 2 + 1, :] = v[1 + f : 2 + f]

    beyond_pass(whi, wlo, (ft,), part, finish)


def call(body, outs, operands, scratch=(), limit=12 << 20, flops=0, first=None, **static):
    def named(*refs):
        body(*refs, **static)

    specs = [VMEM] * len(operands)
    if first is not None:
        specs[0] = first
    return pl.pallas_call(
        named,
        out_shape=outs,
        in_specs=specs,
        out_specs=jax.tree.map(lambda o: SMEM if o.shape == (ITERS,) else VMEM, outs),
        scratch_shapes=list(scratch),
        compiler_params=pltpu.CompilerParams(vmem_limit_bytes=limit),
        cost_estimate=pl.CostEstimate(flops=flops, transcendentals=0, bytes_accessed=0) if flops else None,
    )(*operands)


def sds(*shape, dtype=F32):
    return jax.ShapeDtypeStruct(shape, dtype)


def on_device(positions, velocities, pressure_prev, counts, out_positions, out_velocities, out_dir, out_cell, out_count):
    pairs, plane = lax.axis_size("gx0"), lax.axis_size("gy") * lax.axis_size("gz")
    group = 2 * plane
    across = [(2 * j + 1, 2 * j + 2) for j in range(pairs - 1)]
    across = across + [(b, a) for a, b in across]
    busy = 4 * 10**9

    def spread(send):
        return lax.all_to_all(send, GROUP, 0, 0)

    def from_beyond(layer):
        return lax.ppermute(layer, ("gx0", "gx1"), across)

    def layers(send, mine, shape):
        return call(gather_kernel, (sds(16, *shape),) * 3, (spread(send), mine))

    def features(columns):
        return pltpu.VMEM((columns, 32, 512), BF16)

    tiles, rows = sds(8, 8, 128), sds(8, 128)
    send, one = call(
        pack_kernel,
        (sds(group, 8, 128), rows),
        (out_count, out_positions, out_velocities, out_dir, out_cell),
        limit=60 * 1024 * 1024,
        first=SMEM,
    )
    base, before, filled = call(
        prepare_kernel, (tiles, rows, rows), (positions, velocities, pressure_prev, counts), flops=busy // 4
    )
    chunks, cells = sds(group, 4, 4, 128), sds(8, 4, 128)
    send, state, mine = call(
        insert_kernel, (chunks, tiles, cells), (spread(send), from_beyond(one), base, filled)
    )
    l1, l2, near = layers(send, mine, (4, 128))
    beyond = from_beyond(l1)
    wmain, wside = sds(2, 2, 15, 384, 128, dtype=BF16), sds(2, 2, 3, 384, 128, dtype=BF16)
    whi, wlo, xr, own, bside, dpart, gpart = call(
        setup_main_kernel,
        (wmain, wmain, sds(48, 8, 128), tiles, sds(2, 64, 256, dtype=BF16), tiles, tiles),
        (l1, l2, near, state),
        [pltpu.VMEM((12, 512, 64), BF16), pltpu.VMEM((4, 64, 256), BF16)],
        flops=3 * busy,
    )
    bhi, blo, xrb, gsq, safe2, press, send, mine = call(
        setup_beyond_kernel,
        (wside, wside, sds(16, 8, 128), tiles, rows, rows, chunks, cells),
        (beyond, own, bside, dpart, gpart, filled, before),
        [pltpu.VMEM((4, 512, 64), BF16), pltpu.VMEM((8, 8, 128), F32)],
    )
    errs = None
    for it in range(ITERS):
        last = it == ITERS - 1
        l1, l2, near = layers(send, mine, (128,) if it else (4, 128))
        beyond = from_beyond(l1)
        if it == 0:
            (part,) = call(
                first_main_kernel, (sds(8, 16, 128),), (l1, l2, near, xr, whi, wlo), [features(12)] * 2, flops=busy
            )
            send, mine, grad, aux = call(
                first_accel_kernel,
                (chunks, cells, tiles, tiles),
                (beyond, xrb, bhi, blo, part, l1, l2, xr, own, gsq, safe2),
                [features(4)] * 2,
            )
        else:
            (part,) = call(
                main_kernel, (tiles,), (l1, l2, near, xr, whi, wlo), [features(12)], flops=busy, features=scaled_features
            )
            send, mine = call(
                accel_kernel, (chunks, cells), (beyond, xrb, bhi, blo, part, l1, l2, xr, grad), [features(4)]
            )
        l1, l2, near = layers(send, mine, (4, 128))
        beyond = from_beyond(l1)
        (part,) = call(
            main_kernel, (tiles,), (l1, l2, near, xr, whi, wlo), [features(12)], flops=busy, features=accel_features
        )

        def body(*refs, it=it, last=last):
            refs = refs if it else (*refs[:11], None, *refs[11:])
            apply_kernel(*refs, at_iter=it, last=last)

        operands = (beyond, xrb, bhi, blo, part, l1, l2, xr, grad, aux, press) + (() if it == 0 else (errs,))
        press, errs, send, mine = call(
            body,
            (sds(2, 2, 2, 128) if last else rows, rows, sds(group, 16 if last else 4, 128), rows),
            operands,
            [features(4)],
        )
    send, l1, l2, near, _ = call(
        gather_last_kernel, (sds(pairs, 24, 128),) + (sds(16, 128),) * 4, (spread(send), mine)
    )
    recv = lax.all_to_all(send, "gx0", 0, 0)
    (part,) = call(
        main_kernel, (tiles,), (l1, l2, near, xr, whi, wlo), [features(12)], flops=busy, features=scaled_features
    )
    velocity_new, density_error = call(
        final_kernel,
        (sds(3, 2, 2, 2, 128), sds(ITERS)),
        (recv, xrb, bhi, blo, part, l1, l2, xr, grad, state),
        [pltpu.VMEM((16, 128), F32), features(4)],
        slots=pairs * group * 8 * 128,
    )
    return press, velocity_new, density_error


def solution(mesh):
    nx, ny, nz = (mesh.shape[a] for a in ("gx", "gy", "gz"))
    paired = Mesh(mesh.devices.reshape(nx // 2, 2, ny, nz), ("gx0", "gx1", "gy", "gz"))
    gx = ("gx0", "gx1")
    cells = P(gx, "gy", "gz", None)
    vectors = P(None, gx, "gy", "gz", None)
    ints = P(gx, "gy", "gz")
    return jax.shard_map(
        on_device,
        mesh=paired,
        in_specs=(vectors, vectors, cells, ints, vectors, vectors, cells, cells, ints),
        out_specs=(cells, vectors, P()),
        check_vma=False,
    )
```
